32 devices in a mesh: gz: 16 (over z, x, core), gy: 2 (over y).
Axes of the slice: x: 2, y: 2, z: 4, core: 2. Of those that a mesh axis runs over, the one named last changes fastest.
Arguments:
- spread_weights: float32 [64, 32768], P(None, ('gz', 'gy')), may hold values from -6 to 6
- spread_base: int32 [3, 32768], P(None, ('gz', 'gy')), may hold values from 0 to 383, as said below
- qm_base: int32 [3, 4096], P(None, ('gz', 'gy')), may hold values from 0 to 383, as said below
- qm_frac: float32 [3, 4096], P(None, ('gz', 'gy')), may hold values from 0 to 1
- qm_charge: float32 [4096], P(('gz', 'gy')), may hold values from -3 to 3
Outputs:
- qm_forces: float32 [3, 4096], P(None, ('gz', 'gy'))
The draws below stay inside these ranges and needn't reach their ends.
Inputs may be any that keep to these rules, and one draw needn't show every extreme that they name: For point charge j let d = j // 1024, p = d // 2 and q = d % 2; then spread_base[0, j] lies in [p * 24, (p + 1) * 24) and spread_base[1, j] in [q * 192, (q + 1) * 192); spread_base[2, j] is any cell. For quantum-region atom i let d = i // 128, p = d // 2 and q = d % 2; then qm_base[0, i] lies in [p * 24, (p + 1) * 24) and qm_base[1, i] in [q * 192, (q + 1) * 192); qm_base[2, i] is any cell.
All inputs are finite; a program needn't handle non-finite values.
Results may differ from the reference program's by a relative error of at most 0.0003.
Values sent between devices are 32-bit elements; how exact they have to be, the bound alone decides.
A program may use at most 256 MiB of HBM per device.

```python
import math
import jax
import jax.numpy as jnp

GRID = 384
ORDER = 4
ATOMS_DEV = 1024
QM_DEV = 128
ZLOC = 24
YLOC = 192
ATOMS = 32768
QMS = 4096


def place_bases(key, total, per_device):
    index = jnp.arange(total, dtype=jnp.int32)
    device = index // per_device
    groups = GRID // YLOC
    z_part = device // groups
    y_part = device % groups
    key_z, key_y, key_x = jax.random.split(key, 3)
    first_z = z_part * ZLOC + jax.random.randint(key_z, (total,), 0, ZLOC, dtype=jnp.int32)
    first_y = y_part * YLOC + jax.random.randint(key_y, (total,), 0, YLOC, dtype=jnp.int32)
    first_x = jax.random.randint(key_x, (total,), 0, GRID, dtype=jnp.int32)
    return jnp.stack([first_z, first_y, first_x]).astype(jnp.int32)


def draw_spread_base(key, part):
    return place_bases(jax.random.fold_in(key, 11), ATOMS, ATOMS_DEV)


def draw_qm_base(key, part):
    return place_bases(jax.random.fold_in(key, 23), QMS, QM_DEV)


def block_scale(own_key, extent, cuts, low, top_value):
    loudness, own = 1.0, jax.random.fold_in(own_key, 6)
    for position, blocks in cuts:
        draws = jnp.exp(jax.random.uniform(jax.random.fold_in(own, position), (blocks,), jnp.float32, low / len(cuts), top_value / len(cuts)))
        loudness = loudness * jnp.repeat(draws, extent[position] // blocks).reshape([-1 if axis == position else 1 for axis in range(len(extent))])
    return loudness


def normal_values(rng, shape, deviation, limit, shards=(), kind=jnp.bfloat16):
    drawn = jax.random.normal(rng, shape, jnp.float32) * deviation
    if len(shards) > 0:
        drawn = block_scale(rng, shape, shards, -0.22, 0.18) * drawn
    return jnp.clip(drawn, min=-limit, max=limit).astype(kind)


def setup_inputs(seed: int = 0) -> dict:
    keys = jax.random.split(jax.random.key(seed), 6)
    return {
        "spread_weights": normal_values(keys[0], (ORDER * ORDER * ORDER, ATOMS), 1.0, 6.0, ((1, 32),), jnp.float32),
        "spread_base": draw_spread_base(jax.random.fold_in(keys[5], 71), 0),
        "qm_base": draw_qm_base(jax.random.fold_in(keys[5], 71), 0),
        "qm_frac": jnp.clip(1.0 * jax.random.uniform(keys[3], (3, QMS), jnp.float32) ** block_scale(keys[3], (3, QMS), ((1, 32),), -0.2, 0.2), 0.0, 1.0),
        "qm_charge": normal_values(keys[4], (QMS,), 0.5, 3.0, ((0, 32),), jnp.float32),
    }


SPLITTING = 0.8


def moduli(index, points):
    signed = jnp.where(index < points // 2, index, index - points).astype(jnp.float32) / points
    spline = 2.0 / 3.0 + jnp.cos((2.0 * math.pi / points) * index.astype(jnp.float32)) / 3.0
    return signed * signed, 1.0 / (spline * spline), index == points // 2


def influence(first, second, third, points):
    sq_one, mod_one, edge_one = moduli(first, points)
    sq_two, mod_two, edge_two = moduli(second, points)
    sq_three, mod_three, edge_three = moduli(third, points)
    total = sq_one + sq_two + sq_three
    safe = jnp.where(total > 0.0, total, 1.0)
    value = mod_one * mod_two * mod_three * jnp.exp(-(math.pi * math.pi / (SPLITTING * SPLITTING)) * total) / (math.pi * safe)
    keep = (total > 0.0) & jnp.logical_not(edge_one | edge_two | edge_three)
    return jnp.where(keep, value, 0.0)


def spline_weights(frac):
    remain = 1.0 - frac
    square = frac * frac
    cubed = square * frac
    values = jnp.stack([remain * remain * remain / 6.0, (3.0 * cubed - 6.0 * square + 4.0) / 6.0,
                        (-3.0 * cubed + 3.0 * square + 3.0 * frac + 1.0) / 6.0, cubed / 6.0])
    slopes = jnp.stack([-0.5 * remain * remain, (3.0 * square - 4.0 * frac) / 2.0,
                        (-3.0 * square + 2.0 * frac + 1.0) / 2.0, 0.5 * square])
    return values, slopes


def forces_from(patch, qm_frac, qm_charge):
    w_z, d_z = spline_weights(qm_frac[0])
    w_y, d_y = spline_weights(qm_frac[1])
    w_x, d_x = spline_weights(qm_frac[2])

    def contract(first, second, third):
        return jnp.sum(patch * (first[:, None, None, :] * second[None, :, None, :] * third[None, None, :, :]), axis=(0, 1, 2))

    return jnp.stack([-qm_charge * contract(d_z, w_y, w_x), -qm_charge * contract(w_z, d_y, w_x),
                      -qm_charge * contract(w_z, w_y, d_x)])


def reference(spread_weights, spread_base, qm_base, qm_frac, qm_charge):
    points = GRID
    offsets = jnp.arange(ORDER * ORDER * ORDER, dtype=jnp.int32)
    off_z = offsets // (ORDER * ORDER)
    off_y = (offsets // ORDER) % ORDER
    off_x = offsets % ORDER
    flat_index = (((spread_base[0][None, :] + off_z[:, None]) % points) * points
                  + (spread_base[1][None, :] + off_y[:, None]) % points) * points + (spread_base[2][None, :] + off_x[:, None]) % points
    charge = jnp.zeros((points * points * points,), jnp.float32).at[flat_index.reshape(-1)].add(spread_weights.reshape(-1))
    charge = charge.reshape(points, points, points)
    spectrum = jnp.fft.fftn(charge)
    index = jnp.arange(points, dtype=jnp.int32)
    green = influence(index[:, None, None], index[None, :, None], index[None, None, :], points)
    potential = jnp.real(jnp.fft.ifftn(spectrum * green)).astype(jnp.float32)
    shifts_up = jnp.arange(ORDER, dtype=jnp.int32)[:, None]
    cell_z = (qm_base[0][None, :] + shifts_up) % points
    cell_y = (qm_base[1][None, :] + shifts_up) % points
    cell_x = (qm_base[2][None, :] + shifts_up) % points
    patch = potential[cell_z[:, None, None, :], cell_y[None, :, None, :], cell_x[None, None, :, :]]
    return forces_from(patch, qm_frac, qm_charge)
```

```python
import functools
import math

import jax
import jax.numpy as jnp
import numpy as np
from jax import lax
from jax.experimental import pallas as pl
from jax.experimental.pallas import tpu as pltpu
from jax.sharding import PartitionSpec as P

GRID = 384
ORDER = 4


SPLITTING = 0.8
HIGHEST = lax.Precision.HIGHEST
HIGH = lax.Precision.HIGH
GROUP = 64


def moduli(index, points):
    signed = jnp.where(index < points // 2, index, index - points).astype(jnp.float32) / points
    spline = 2.0 / 3.0 + jnp.cos(2.0 * math.pi / points * index.astype(jnp.float32)) / 3.0
    return (signed * signed, 1.0 / (spline * spline), index == points // 2)


def influence(first, second, third, points):
    sq_one, mod_one, edge_one = moduli(first, points)
    sq_two, mod_two, edge_two = moduli(second, points)
    sq_three, mod_three, edge_three = moduli(third, points)
    total = sq_one + sq_two + sq_three
    safe = jnp.where(total > 0.0, total, 1.0)
    value = (
        mod_one
        * mod_two
        * mod_three
        * jnp.exp(-(math.pi * math.pi / (SPLITTING * SPLITTING)) * total)
        / (math.pi * safe)
    )
    keep = (total > 0.0) & jnp.logical_not(edge_one | edge_two | edge_three)
    return jnp.where(keep, value, 0.0)


def spline_weights(frac):
    remain = 1.0 - frac
    square = frac * frac
    cubed = square * frac
    values = jnp.stack(
        [
            remain * remain * remain / 6.0,
            (3.0 * cubed - 6.0 * square + 4.0) / 6.0,
            (-3.0 * cubed + 3.0 * square + 3.0 * frac + 1.0) / 6.0,
            cubed / 6.0,
        ]
    )
    slopes = jnp.stack(
        [
            -0.5 * remain * remain,
            (3.0 * square - 4.0 * frac) / 2.0,
            (-3.0 * square + 2.0 * frac + 1.0) / 2.0,
            0.5 * square,
        ]
    )
    return (values, slopes)


def angle_tables(rows_in, cols_in, points):
    product = rows_in[:, None] * cols_in[None, :] % points
    angle = 2.0 * math.pi / points * product.astype(jnp.float32)
    return (jnp.cos(angle), jnp.sin(angle))


def line_tables(cells, values, slopes, extent):
    hits = (jnp.arange(extent, dtype=jnp.int32)[None, :, None] == cells[:, None, :]).astype(
        jnp.float32
    )
    return (jnp.sum(hits * values[:, None, :], axis=0), jnp.sum(hits * slopes[:, None, :], axis=0))


def spread_kernel(first_ref, count_ref, weights_ref, z_ref, y_ref, waves_ref, out_ref):
    half = pl.program_id(0)
    group = pl.program_id(1)

    @pl.when(group == 0)
    def _():
        out_ref[...] = jnp.zeros_like(out_ref)

    rows = out_ref.shape[1]
    weights = weights_ref[...]
    z_cell = z_ref[...]
    y_cell = y_ref[...]
    waves = waves_ref[...]
    high = waves.astype(jnp.bfloat16)
    low = (waves - high.astype(jnp.float32)).astype(jnp.bfloat16)
    first = first_ref[half, group]
    row_offset = lax.broadcasted_iota(jnp.int32, (rows, weights.shape[1]), 0) - y_cell

    def plane(step, carry):
        z = first + step
        offset = z - z_cell
        chosen = jnp.zeros((ORDER, weights.shape[1]), jnp.float32)
        for a in range(ORDER):
            chosen = jnp.where(offset == a, weights[a * ORDER : (a + 1) * ORDER], chosen)
        placed = jnp.zeros((rows, weights.shape[1]), jnp.float32)
        for b in range(ORDER):
            placed = jnp.where(row_offset == b, chosen[b : b + 1], placed)
        top = placed.astype(jnp.bfloat16)
        rest = (placed - top.astype(jnp.float32)).astype(jnp.bfloat16)
        total = jnp.dot(top, high, preferred_element_type=jnp.float32)
        total += jnp.dot(rest, high, preferred_element_type=jnp.float32)
        total += jnp.dot(top, low, preferred_element_type=jnp.float32)
        out_ref[z] += total
        return carry

    lax.fori_loop(0, count_ref[half, group], plane, 0)


def sort_by_plane(table, local_z):
    count = local_z.shape[0]
    order = jnp.arange(count, dtype=jnp.int32)
    before = (local_z[:, None] < local_z[None, :]) | (
        (local_z[:, None] == local_z[None, :]) & (order[:, None] < order[None, :])
    )
    rank = jnp.sum(before.astype(jnp.int32), axis=0)
    moves = (rank[:, None] == order[None, :]).astype(jnp.float32)
    return jnp.dot(table, moves, precision=HIGHEST)


def phases(cells, index, points):
    angle = (2.0 * math.pi / points) * (cells[..., None] * index % points).astype(jnp.float32)
    return (jnp.cos(angle), jnp.sin(angle))


def spread_lines(spread_weights, spread_base, z_first, y_first, z_extent, y_local, kx_index, points):
    count = spread_weights.shape[1]
    halves = lax.axis_size("gy")
    local = jnp.stack([spread_base[0] - z_first, spread_base[1] - y_first, spread_base[2]])
    table = jnp.concatenate([spread_weights, local.astype(jnp.float32)], axis=0)
    table = sort_by_plane(table, local[0])
    table = lax.all_gather(table, "gy")
    groups = count // GROUP
    width = ORDER * GROUP
    weights = table[:, : ORDER**3].reshape(halves, ORDER * ORDER, ORDER, groups, GROUP)
    weights = weights.transpose(0, 3, 1, 2, 4).reshape(halves, groups, ORDER * ORDER, width)
    cells = jnp.round(table[:, ORDER**3 :]).astype(jnp.int32).reshape(halves, 3, groups, GROUP)
    z_cell, y_cell, x_cell = cells[:, 0], cells[:, 1], cells[:, 2]
    first = jnp.min(z_cell, axis=-1)
    planes = jnp.max(z_cell, axis=-1) - first + ORDER
    z_wide = jnp.tile(z_cell, (1, 1, ORDER))[:, :, None, :]
    y_wide = jnp.tile(y_cell, (1, 1, ORDER))[:, :, None, :]
    cosine, sine = phases(x_cell, kx_index, points)
    step_cos, step_sin = phases(jnp.arange(ORDER, dtype=jnp.int32), kx_index, points)
    step_cos, step_sin = step_cos[:, None, :], step_sin[:, None, :]
    cosine, sine = cosine[:, :, None], sine[:, :, None]
    waves = jnp.concatenate(
        [cosine * step_cos - sine * step_sin, -(sine * step_cos + cosine * step_sin)], axis=-1
    ).reshape(halves, groups, width, -1)
    rows = -(-(y_local + ORDER - 1) // 8) * 8
    lanes = waves.shape[-1]
    per_group = lambda q, g, *_: (q, g, 0, 0)
    lines = pl.pallas_call(
        spread_kernel,
        grid_spec=pltpu.PrefetchScalarGridSpec(
            num_scalar_prefetch=2,
            grid=(halves, groups),
            in_specs=[
                pl.BlockSpec((None, None, ORDER * ORDER, width), per_group),
                pl.BlockSpec((None, None, 1, width), per_group),
                pl.BlockSpec((None, None, 1, width), per_group),
                pl.BlockSpec((None, None, width, lanes), per_group),
            ],
            out_specs=pl.BlockSpec((z_extent, None, rows, lanes), lambda q, g, *_: (0, q, 0, 0)),
        ),
        out_shape=jax.ShapeDtypeStruct((z_extent, halves, rows, lanes), jnp.float32),
        compiler_params=pltpu.CompilerParams(dimension_semantics=("arbitrary", "arbitrary")),
    )(first, planes, weights, z_wide, y_wide, waves)
    return lines, rows


def line_waves(cell, values, slopes, index, points):
    cosine, sine = phases(cell, index, points)
    step_cos, step_sin = phases(jnp.arange(ORDER, dtype=jnp.int32), index, points)
    found = []
    for table in (values, slopes):
        real = sum(table[c][..., None] * step_cos[c] for c in range(ORDER))
        imag = sum(table[c][..., None] * step_sin[c] for c in range(ORDER))
        found.append((cosine * real - sine * imag, cosine * imag + sine * real))
    return found


def slab_forces(lines, base, frac, z_first, y_index, x_index, points):
    z_extent, ky_local, _, kx_local = lines.shape
    shifts = jnp.arange(ORDER, dtype=jnp.int32)[:, None]
    w_z, d_z = spline_weights(frac[0])
    w_y, d_y = spline_weights(frac[1])
    w_x, d_x = spline_weights(frac[2])
    plane_w, plane_d = line_tables(base[0][None, :] - z_first + shifts, w_z, d_z, z_extent)
    (wy_re, wy_im), (dy_re, dy_im) = line_waves(base[1], w_y, d_y, y_index, points)
    (wx_re, wx_im), (dx_re, dx_im) = line_waves(base[2], w_x, d_x, x_index, points)
    join = lambda a, b: jnp.concatenate([a, b], axis=1)
    waves = jnp.stack([join(wx_re, -wx_im), join(wx_im, wx_re), join(dx_re, -dx_im), join(dx_im, dx_re)])
    count = base.shape[1]
    along = jnp.einsum(
        "mk,nk->mn",
        lines.reshape(z_extent * ky_local, 2 * kx_local),
        waves.reshape(4 * count, 2 * kx_local),
        precision=HIGH,
    ).reshape(z_extent, ky_local, 4, count)
    wy_re, wy_im, dy_re, dy_im = wy_re.T, wy_im.T, dy_re.T, dy_im.T
    plain = jnp.sum(along[:, :, 0] * wy_re - along[:, :, 1] * wy_im, axis=1)
    tilted = jnp.sum(along[:, :, 0] * dy_re - along[:, :, 1] * dy_im, axis=1)
    sloped = jnp.sum(along[:, :, 2] * wy_re - along[:, :, 3] * wy_im, axis=1)
    return jnp.stack(
        [
            jnp.sum(plain * plane_d, axis=0),
            jnp.sum(tilted * plane_w, axis=0),
            jnp.sum(sloped * plane_w, axis=0),
        ]
    )


def shards(spread_weights, spread_base, qm_base, qm_frac, qm_charge):
    points = GRID
    margin = ORDER - 1
    count_z = lax.axis_size("gz")
    count_y = lax.axis_size("gy")
    z_local = points // count_z
    y_local = points // count_y
    z_extent = z_local + margin
    kx_count = points // 2
    kx_local = kx_count // count_y
    ky_local = points // count_z
    z_first = lax.axis_index("gz") * z_local
    y_first = lax.axis_index("gy") * y_local
    ky_index = lax.axis_index("gz") * ky_local + jnp.arange(ky_local, dtype=jnp.int32)
    kx_index = lax.axis_index("gy") * kx_local + jnp.arange(kx_local, dtype=jnp.int32)
    positions = jnp.arange(points, dtype=jnp.int32)
    all_base = lax.all_gather(qm_base, ("gz", "gy"), axis=1, tiled=True)
    all_frac = lax.all_gather(qm_frac, ("gz", "gy"), axis=1, tiled=True)

    lines, rows = spread_lines(
        spread_weights, spread_base, z_first, y_first, z_extent, y_local, kx_index, points
    )
    row_cells = (
        jnp.arange(count_y, dtype=jnp.int32)[:, None] * y_local
        + jnp.arange(rows, dtype=jnp.int32)[None, :]
    ).reshape(-1) % points
    tables = jnp.concatenate(angle_tables(positions, row_cells, points), axis=0)
    lines = lines.reshape(z_extent, count_y * rows, 2 * kx_local)
    both = jnp.einsum("yr,zrk->zyk", tables, lines, precision=HIGH)
    with_cos, with_sin = both[:, :points], both[:, points:]
    packed = jnp.stack(
        [
            with_cos[:, :, :kx_local] + with_sin[:, :, kx_local:],
            with_cos[:, :, kx_local:] - with_sin[:, :, :kx_local],
        ],
        axis=1,
    )
    packed = packed.reshape(z_extent, 2, count_z, ky_local, kx_local).transpose(2, 0, 1, 3, 4)
    packed = packed.reshape(count_z, z_extent * 2 * ky_local * kx_local)
    moved = lax.all_to_all(packed, "gz", split_axis=0, concat_axis=0, tiled=True)

    z_cells = (
        jnp.arange(count_z, dtype=jnp.int32)[:, None] * z_local
        + jnp.arange(z_extent, dtype=jnp.int32)[None, :]
    ).reshape(-1) % points
    cells = ky_local * kx_local
    moved = moved.reshape(count_z * z_extent, 2 * cells)
    tables = jnp.concatenate(angle_tables(positions, z_cells, points), axis=0)
    both = jnp.dot(tables, moved, precision=HIGH).reshape(2, points, 2, ky_local, kx_local)
    green = influence(
        positions[:, None, None], ky_index[None, :, None], kx_index[None, None, :], points
    )
    kx_weight = jnp.where(kx_index == 0, 1.0, 2.0).astype(jnp.float32)
    green = green * (kx_weight * (1.0 / float(points * points * points)))
    spectrum = jnp.stack(
        [(both[0, :, 0] + both[1, :, 1]) * green, (both[0, :, 1] - both[1, :, 0]) * green], axis=1
    ).reshape(points, 2 * cells)
    back = jnp.concatenate(angle_tables(z_cells, positions, points), axis=0)
    both = jnp.dot(back, spectrum, precision=HIGH)
    both = both.reshape(2, count_z, z_extent, 2, ky_local, kx_local)
    lines = jnp.stack(
        [both[0, :, :, 0] - both[1, :, :, 1], both[0, :, :, 1] + both[1, :, :, 0]], axis=3
    )

    def one_slab(args):
        slab, base, frac, start = args
        return slab_forces(slab, base, frac, start, ky_index, kx_index, points)

    slab_base = all_base.reshape(3, count_z, -1).transpose(1, 0, 2)
    slab_frac = all_frac.reshape(3, count_z, -1).transpose(1, 0, 2)
    starts = jnp.arange(count_z, dtype=jnp.int32) * z_local
    partial = lax.map(one_slab, (lines, slab_base, slab_frac, starts))
    forces = lax.psum_scatter(
        partial.transpose(1, 0, 2).reshape(3, -1), ("gz", "gy"), scatter_dimension=1, tiled=True
    )
    return -qm_charge * forces


MESH = pl.DeviceIdType.MESH
RING = 4
PLANE = 4
LANES = 128
F32 = jnp.float32
BF16 = jnp.bfloat16
VMEM_LIMIT = 62 * 2**20


def split_table(table):
    high = table.astype(np.float32).astype(BF16)
    low = (table - high.astype(np.float64)).astype(np.float32).astype(BF16)
    return jnp.asarray(high), jnp.asarray(low)


def split(value):
    high = value.astype(BF16)
    return high, (value - high.astype(F32)).astype(BF16)


def dot3(a_high, a_low, b_high, b_low):
    total = jnp.dot(a_high, b_high, preferred_element_type=F32)
    total += jnp.dot(a_low, b_high, preferred_element_type=F32)
    return total + jnp.dot(a_high, b_low, preferred_element_type=F32)


def trig(units, points):
    rest = units - points * jnp.floor((units + 0.5) * (1.0 / points))
    quarter = points // 4
    turn = jnp.floor((rest + quarter / 2) * (1.0 / quarter))
    angle = (rest - quarter * turn) * (2.0 * math.pi / points)
    square = angle * angle
    sine = angle * (1.0 + square * (-1.0 / 6 + square * (1.0 / 120 + square * (-1.0 / 5040 + square / 362880))))
    cosine = 1.0 + square * (-0.5 + square * (1.0 / 24 + square * (-1.0 / 720 + square * (1.0 / 40320))))
    odd = (turn == 1.0) | (turn == 3.0)
    first = jnp.where(odd, sine, cosine)
    second = jnp.where(odd, cosine, sine)
    first = jnp.where((turn == 1.0) | (turn == 2.0), -first, first)
    second = jnp.where((turn == 2.0) | (turn == 3.0), -second, second)
    return first, second


def wave_units(lane, kx_first, kx_local):
    sine = lane >= kx_local
    index = jnp.where(sine, lane - kx_local, lane)
    index = jnp.where(index >= kx_local, 0, index)
    return (kx_first + index).astype(F32), sine


def order_by(key, table):
    count = key.shape[0]
    order = jnp.arange(count, dtype=jnp.int32)
    before = (key[:, None] < key[None, :]) | ((key[:, None] == key[None, :]) & (order[:, None] < order[None, :]))
    rank = jnp.sum(before.astype(jnp.int32), axis=0)
    moves = (rank[:, None] == order[None, :]).astype(F32)
    return jnp.dot(table, moves, precision=HIGHEST)


def gather_kernel(count_z, count_y, own_ref, halo_ref, qm_ref, tab_ref, all_ref, own_send, own_recv, halo_send, halo_recv, qm_send, qm_recv):
    p = lax.axis_index("gz")
    y = lax.axis_index("gy")
    me = p * count_y + y
    total = count_z * count_y
    barrier = pltpu.get_barrier_semaphore()
    for d in range(1, total):
        other = lax.rem(me + d, total)
        pl.semaphore_signal(barrier, inc=1, device_id=(other // count_y, lax.rem(other, count_y)), device_id_type=MESH)
    pl.semaphore_wait(barrier, total - 1)
    copies = []

    def send(src, dst, s, r, device):
        copy = pltpu.make_async_remote_copy(src_ref=src, dst_ref=dst, send_sem=s, recv_sem=r, device_id=device, device_id_type=MESH)
        copy.start()
        copies.append(copy)

    upper = lax.rem(p + 1, count_z)
    send(own_ref, tab_ref.at[y, 0], own_send, own_recv, (p, 1 - y))
    send(halo_ref, tab_ref.at[y, 1], halo_send.at[0], halo_recv.at[0], (upper, y))
    send(halo_ref, tab_ref.at[y, 1], halo_send.at[1], halo_recv.at[1], (upper, 1 - y))
    whole = len(copies)
    for d in range(1, total):
        other = lax.rem(me + d, total)
        send(qm_ref, all_ref.at[me], qm_send, qm_recv, (other // count_y, lax.rem(other, count_y)))
    tab_ref[y, 0] = own_ref[...]
    all_ref[me] = qm_ref[...]
    for copy in copies[:whole]:
        copy.wait()
    rest = pltpu.make_async_remote_copy(
        src_ref=all_ref.at[pl.ds(0, total - 1)], dst_ref=all_ref.at[pl.ds(0, total - 1)],
        send_sem=qm_send, recv_sem=qm_recv, device_id=(p, 1 - y), device_id_type=MESH)
    rest.wait()


def gather(own, halo, qm, count_z, count_y):
    vmem = pl.BlockSpec(memory_space=pltpu.VMEM)
    dma = pltpu.SemaphoreType.DMA
    return pl.pallas_call(
        functools.partial(gather_kernel, count_z, count_y),
        out_shape=(
            jax.ShapeDtypeStruct((count_y, 2) + own.shape, F32),
            jax.ShapeDtypeStruct((count_z * count_y,) + qm.shape, F32),
        ),
        in_specs=[vmem] * 3,
        out_specs=(vmem, vmem),
        scratch_shapes=[dma, dma, dma((2,)), dma((2,)), dma, dma],
        compiler_params=pltpu.CompilerParams(collective_id=0, has_side_effects=True, vmem_limit_bytes=VMEM_LIMIT),
        name="gather_atoms",
    )(own, halo, qm)


def lines_kernel(points, kx_local, kx_ref, first_ref, count_ref, tab_ref, out_ref, placed_ref, high_ref, low_ref):
    half, seg, block = pl.program_id(0), pl.program_id(1), pl.program_id(2)
    blocks = pl.num_programs(2)

    @pl.when((seg == 0) & (block == 0))
    def _():
        out_ref[...] = jnp.zeros_like(out_ref)

    lane = lax.broadcasted_iota(jnp.int32, (1, LANES), 1)
    wide = lax.broadcasted_iota(jnp.int32, (1, 2 * LANES), 1)
    kx, sine = wave_units(wide, kx_ref[0], kx_local)
    shift = jnp.where(sine, points - points // 4, points).astype(F32)
    z_rows = out_ref.shape[2]
    part = LANES // 2

    def group(h, steps, z_used):
        index = ((half * 2 + seg) * blocks + block) * 2 + h

        @pl.when(count_ref[index] > 0)
        def _():
            tab = tab_ref[...]

            def pair(even, odd):
                if h == 0:
                    return jnp.where(lane < part, even, pltpu.roll(odd, part, 1))
                return jnp.where(lane < part, pltpu.roll(even, part, 1), odd)

            rows = ORDER * ORDER
            weights = jnp.concatenate(
                [pair(tab[0:rows], tab[rows : 2 * rows]), pair(tab[2 * rows : 3 * rows], tab[3 * rows : 4 * rows])], axis=1)
            spots = tab[4 * rows : 4 * rows + 8]
            spots_pair = pair(spots, spots)
            spots_wide = jnp.concatenate([spots_pair, spots_pair], axis=1).astype(jnp.int32)
            z_off = lax.broadcasted_iota(jnp.int32, (z_used, 2 * LANES), 0) - spots_wide[0:1]
            y_cell = spots_wide[1:2]
            for b in range(ORDER):
                chosen = jnp.zeros((z_used, 2 * LANES), F32)
                for a in range(ORDER):
                    chosen = jnp.where(z_off == a, weights[a * ORDER + b : a * ORDER + b + 1], chosen)
                placed_ref[b, 0:z_used] = chosen
            column = jnp.broadcast_to(spots[2:3], (LANES, LANES)).T[h * part : (h + 1) * part]
            column = jnp.concatenate([column, column], axis=1)
            cosine, sinus = trig(kx * column + shift, points)
            step = lax.broadcasted_iota(jnp.int32, (8, 2 * LANES), 0).astype(F32)
            step_cos, step_sin = trig(kx * step, points)
            for c in range(ORDER):
                wave = cosine * step_cos[c : c + 1] - sinus * step_sin[c : c + 1] if c else cosine
                high, low = split(wave)
                high_ref[c * part : (c + 1) * part] = high
                low_ref[c * part : (c + 1) * part] = low
            first = first_ref[index]

            def rows_of(it, carry):
                y_first = first + it * steps
                pieces = []
                for s in range(steps):
                    off = (y_first + s) - y_cell
                    placed = jnp.zeros((z_used, 2 * LANES), F32)
                    for b in range(ORDER):
                        placed = jnp.where(off == b, placed_ref[b, 0:z_used], placed)
                    pieces.append(placed)
                top, rest = split(jnp.concatenate(pieces, axis=0))
                total = dot3(top, rest, high_ref[...], low_ref[...])
                for t in range(2):
                    part_of = total[:, t * LANES : (t + 1) * LANES].reshape(steps, z_used, LANES)
                    out_ref[t, pl.ds(y_first, steps), 0:z_used, :] += part_of
                return carry

            lax.fori_loop(0, count_ref[index], rows_of, 0)

    for h in range(2):

        @pl.when(seg == 0)
        def _():
            group(h, OWN_STEP, z_rows)

        @pl.when(seg == 1)
        def _():
            group(h, HALO_STEP, 8)


OWN_STEP = 16
HALO_STEP = 32


def spread(tab, kx_first, kx_local, z_local, y_local, points):
    halves, segs, rows, count = tab.shape
    extent = -(-(y_local + ORDER - 1 + HALO_STEP - 1) // 8) * 8
    part = LANES // 2
    cells = jnp.round(tab[:, :, 4 * ORDER * ORDER : 4 * ORDER * ORDER + 2]).astype(jnp.int32)
    cells = cells.reshape(halves, segs, 2, count // part, part)
    z_cell, y_cell = cells[:, :, 0], cells[:, :, 1]
    live = z_cell > -ORDER
    low = jnp.min(jnp.where(live, y_cell, points), axis=-1)
    top = jnp.max(jnp.where(live, y_cell, -points), axis=-1) + ORDER
    steps = jnp.asarray([OWN_STEP, HALO_STEP], jnp.int32)[None, :, None]
    counts = jnp.maximum((top - low + steps - 1) // steps, 0)
    return pl.pallas_call(
        functools.partial(lines_kernel, points, kx_local),
        grid_spec=pltpu.PrefetchScalarGridSpec(
            num_scalar_prefetch=3,
            grid=(halves, segs, count // LANES),
            in_specs=[pl.BlockSpec((None, None, rows, LANES), lambda h, s, b, *_: (h, s, 0, b))],
            out_specs=pl.BlockSpec((2, None, extent, z_local, LANES), lambda h, s, b, *_: (0, h, 0, 0, 0)),
            scratch_shapes=[
                pltpu.VMEM((ORDER, z_local, 2 * LANES), F32),
                pltpu.VMEM((2 * LANES, 2 * LANES), BF16),
                pltpu.VMEM((2 * LANES, 2 * LANES), BF16),
            ],
        ),
        out_shape=jax.ShapeDtypeStruct((2, halves, extent, z_local, LANES), F32),
        compiler_params=pltpu.CompilerParams(
            dimension_semantics=("arbitrary",) * 3, vmem_limit_bytes=VMEM_LIMIT),
        name="spread_lines",
    )(kx_first.reshape(1), low.reshape(-1), counts.reshape(-1), tab)


def flip_of(a, b):
    ax, ac = a // 2, lax.rem(a, 2)
    bx, bc = b // 2, b % 2
    return 2 * jnp.abs(ax - bx) + jnp.abs(ac - bc)


def rows_kernel(z_local, groups, here_ref, lines_ref, high_ref, low_ref, out_ref):
    ring, spot = here_ref[0], here_ref[1]
    lane = lax.broadcasted_iota(jnp.int32, (8, LANES), 1)
    deep = lines_ref.shape[1] // z_local
    packed_rows = 12 * groups

    def plane(z, carry):
        data = jnp.concatenate(
            [lines_ref[t, pl.ds(z, deep, stride=z_local), :] for t in range(2)], axis=1)
        high, low = split(data)
        out = dot3(high_ref[...], low_ref[...], high, low)
        for p in range(RING * PLANE):
            slot = lax.rem(p // PLANE - ring + RING, RING) * PLANE + flip_of(spot, p % PLANE)
            for g in range(groups):
                rows = out[(g * RING * PLANE + p) * 8 :][:8]
                base = (slot * packed_rows + g * 12) * z_local + z
                out_ref[pl.ds(base, 8, stride=z_local), :] = rows[:, :LANES]
                tail = rows[:, LANES:]
                tail = jnp.where(lane < LANES // 2, tail, pltpu.roll(pltpu.roll(tail, LANES // 2, 1), 4, 0))
                out_ref[pl.ds(base + 8 * z_local, 4, stride=z_local), :] = tail[:4]
        return carry

    lax.fori_loop(0, z_local, plane, 0)


def transform_rows(lines, here, y_local, points):
    tiles, halves, extent, z_local, width = lines.shape
    parts = RING * PLANE
    block = points // parts
    groups = block // 8
    g, p, r = np.meshgrid(np.arange(groups), np.arange(parts), np.arange(8), indexing="ij")
    ky = ((p // 2) * block + g * 8 + r).reshape(-1)
    sine = (p % 2).reshape(-1)
    cell = (np.arange(halves)[:, None] * y_local + np.arange(extent)[None, :]).reshape(-1) % points
    angle = 2.0 * np.pi / points * ((ky[:, None] * cell[None, :]) % points)
    table = np.where(sine[:, None] == 0, np.cos(angle), np.sin(angle))
    high, low = split_table(table)
    vmem = pl.BlockSpec(memory_space=pltpu.VMEM)
    out = pl.pallas_call(
        functools.partial(rows_kernel, z_local, groups),
        in_specs=[pl.BlockSpec(memory_space=pltpu.SMEM), vmem, vmem, vmem],
        out_specs=vmem,
        out_shape=jax.ShapeDtypeStruct((parts * 12 * groups * z_local, LANES), F32),
        compiler_params=pltpu.CompilerParams(vmem_limit_bytes=VMEM_LIMIT),
        name="transform_rows",
    )(here, lines.reshape(tiles, halves * extent * z_local, width), high, low)
    return out.reshape(RING, PLANE, 12 * groups, z_local, LANES)


CHUNKS = 6


def exchange_kernel(send_ref, out_ref, cross_ref, relay_ref, s_near, r_near, s_cross, r_cross, s_hop, r_hop, s_relay, r_relay, s_last, r_last):
    p = lax.axis_index("gz")
    y = lax.axis_index("gy")
    ring, spot = p // PLANE, lax.rem(p, PLANE)
    x, core = spot // 2, lax.rem(spot, 2)
    spots = [spot, x * 2 + 1 - core, (1 - x) * 2 + core, (1 - x) * 2 + 1 - core]
    up, down = lax.rem(ring + 1, RING), lax.rem(ring + RING - 1, RING)
    above, below = up * PLANE + spot, down * PLANE + spot
    across = [ring * PLANE + s for s in spots]
    rows = send_ref.shape[2] // CHUNKS
    z_local = send_ref.shape[3]
    barrier = pltpu.get_barrier_semaphore()
    for other in across[1:] + [above, below]:
        pl.semaphore_signal(barrier, inc=1, device_id=(other, y), device_id_type=MESH)
    pl.semaphore_wait(barrier, PLANE + 1)

    def copy(src, dst, s, r, device):
        return pltpu.make_async_remote_copy(src_ref=src, dst_ref=dst, send_sem=s, recv_sem=r, device_id=(device, y), device_id_type=MESH)

    def span(j):
        return pl.ds(j * rows, rows)

    def held(d, z, j):
        return send_ref.at[z, 0, span(j)] if d == 0 else cross_ref.at[d - 1, z - 1, span(j)]

    for j in range(CHUNKS):
        for d in (2, 3, 1):
            copy(send_ref.at[pl.ds(1, RING - 1), d, span(j)], cross_ref.at[d - 1, :, span(j)], s_cross.at[j], r_cross.at[j], across[d]).start()
    for j in range(CHUNKS):
        for d in (2, 3, 1):
            copy(send_ref.at[0, d, span(j)], out_ref.at[span(j), p], s_near.at[j], r_near.at[j], across[d]).start()
    for i in range(out_ref.shape[0]):
        out_ref[i, p] = send_ref[0, 0, i]
    big = lambda j: cross_ref.at[:, :, span(j)]
    three = lambda j: cross_ref.at[0, :, span(j)]
    four = lambda j: relay_ref.at[:, span(j)]
    eight = lambda j: send_ref.at[pl.ds(0, 2), :, span(j)]

    def hop(j):
        copy(big(j), big(j), s_cross.at[j], r_cross.at[j], above).wait_recv()
        for d in (0, 1, 2, 3):
            copy(held(d, 2, j), relay_ref.at[d, span(j)], s_relay.at[j], r_relay.at[j], above if d < 2 else below).start()
        for d in (0, 1, 2, 3):
            copy(held(d, 1, j), out_ref.at[span(j), across[d]], s_hop.at[j], r_hop.at[j], above).start()
            copy(held(d, 3, j), out_ref.at[span(j), across[d]], s_hop.at[j], r_hop.at[j], below).start()

    def forward(j):
        copy(four(j), four(j), s_relay.at[j], r_relay.at[j], above).wait_recv()
        for d in (0, 1, 2, 3):
            origin = (down if d < 2 else up) * PLANE + spots[d]
            copy(relay_ref.at[d, span(j)], out_ref.at[span(j), origin], s_last.at[j], r_last.at[j], above if d < 2 else below).start()

    def finish(j):
        copy(three(j), three(j), s_near.at[j], r_near.at[j], above).wait_recv()
        copy(eight(j), eight(j), s_hop.at[j], r_hop.at[j], above).wait_recv()
        copy(four(j), four(j), s_last.at[j], r_last.at[j], above).wait_recv()

    for j in range(CHUNKS):
        hop(j)
        if j >= 1:
            forward(j - 1)
    forward(CHUNKS - 1)
    for j in range(CHUNKS):
        finish(j)
    for j in range(CHUNKS):
        copy(big(j), big(j), s_cross.at[j], r_cross.at[j], above).wait_send()
        copy(three(j), three(j), s_near.at[j], r_near.at[j], above).wait_send()
        copy(four(j), four(j), s_relay.at[j], r_relay.at[j], above).wait_send()
        copy(eight(j), eight(j), s_hop.at[j], r_hop.at[j], above).wait_send()
        copy(four(j), four(j), s_last.at[j], r_last.at[j], above).wait_send()


def exchange(send):
    ring, plane, rows, z_local, lanes = send.shape
    vmem = pl.BlockSpec(memory_space=pltpu.VMEM)
    return pl.pallas_call(
        exchange_kernel,
        in_specs=[vmem],
        out_specs=vmem,
        out_shape=jax.ShapeDtypeStruct((rows, ring * plane, z_local, lanes), F32),
        scratch_shapes=[
            pltpu.VMEM((plane - 1, ring - 1, rows, z_local, lanes), F32),
            pltpu.VMEM((plane, rows, z_local, lanes), F32),
        ] + [pltpu.SemaphoreType.DMA((CHUNKS,))] * 10,
        compiler_params=pltpu.CompilerParams(collective_id=1, has_side_effects=True, vmem_limit_bytes=VMEM_LIMIT),
        name="exchange_blocks",
    )(send)


def solve_kernel(points, kx_local, block, here_ref, x_ref, fh_ref, fl_ref, bh_ref, bl_ref, az_ref, sz_ref, col_ref, sq_ref, step_ref, qm_ref, out_ref, pot_ref, wave_h, wave_l, wy_ref, acc_ref):
    rows = x_ref.shape[0]
    modes = points // 2
    slabs = qm_ref.shape[0]
    z_local = points // slabs
    atoms = qm_ref.shape[2]
    kx_first, ky_first, y_shift = here_ref[0], here_ref[1], here_ref[2]

    def convolve(t, carry):
        pairs = [x_ref[2 * t], x_ref[2 * t + 1]]
        high, low = split(jnp.concatenate(pairs, axis=1))
        coef = dot3(fh_ref[...], fl_ref[...], high, low)
        greens = []
        for i in range(2):
            total = sz_ref[...] + sq_ref[pl.ds(2 * t + i, 1), :]
            keep = total > 0.0
            value = az_ref[...] * col_ref[pl.ds(2 * t + i, 1), :] / jnp.where(keep, total, 1.0)
            greens.append(jnp.where(keep, value, 0.0))
        green = jnp.concatenate(greens, axis=1)
        high, low = split(coef * jnp.concatenate([green, green], axis=0))
        back = dot3(bh_ref[...], bl_ref[...], high, low)
        pot_ref[2 * t] = back[:, :LANES]
        pot_ref[2 * t + 1] = back[:, LANES:]
        return carry

    lax.fori_loop(0, rows // 2, convolve, 0)
    span = 4 * 8
    wave_rows = 2 * kx_local
    wave_h[wave_rows:] = jnp.zeros((2 * LANES - wave_rows, 2 * atoms), BF16)
    wave_l[wave_rows:] = jnp.zeros((2 * LANES - wave_rows, 2 * atoms), BF16)
    kx, sine = wave_units(lax.broadcasted_iota(jnp.int32, (wave_rows, atoms), 0), kx_first, kx_local)
    x_shift = jnp.where(sine, points - points // 4, points).astype(F32)
    ky = (ky_first + lax.broadcasted_iota(jnp.int32, (block, atoms), 0)).astype(F32)

    def slab(p, carry):
        qm = qm_ref[p]
        row = lambda i: qm[i : i + 1]
        cosine, sinus = trig(kx * row(2) + x_shift, points)
        for k, at in ((0, 19), (1, 23)):
            real = imag = None
            for c in range(ORDER):
                sc = jnp.concatenate([step_ref[c, 0:wave_rows]] * (atoms // LANES), axis=1)
                ss = jnp.concatenate([step_ref[ORDER + c, 0:wave_rows]] * (atoms // LANES), axis=1)
                real = row(at + c) * sc if real is None else real + row(at + c) * sc
                imag = row(at + c) * ss if imag is None else imag + row(at + c) * ss
            high, low = split(cosine * real - sinus * imag)
            wave_h[0:wave_rows, k * atoms : (k + 1) * atoms] = high
            wave_l[0:wave_rows, k * atoms : (k + 1) * atoms] = low
        plain_y = slope_y = jnp.zeros((block, atoms), F32)
        for c in range(ORDER):
            wave, _ = trig(ky * (row(1) + float(c)) + y_shift.astype(F32), points)
            plain_y += row(11 + c) * wave
            slope_y += row(15 + c) * wave
        wy_ref[0] = plain_y
        wy_ref[1] = slope_y
        z_first = pl.multiple_of(p * z_local, 8)
        acc_ref[...] = jnp.zeros_like(acc_ref)
        for g in range(block // 8):
            tiles = []
            for i in range(8):
                lead = pot_ref[g * 12 + i, pl.ds(z_first, span), :]
                tail = pot_ref[g * 12 + 8 + i % 4, pl.ds(z_first, span), :]
                if i >= 4:
                    tail = pltpu.roll(tail, LANES // 2, 1)
                tiles.append(jnp.concatenate([lead, tail], axis=1))
            high, low = split(jnp.concatenate(tiles, axis=0))
            along = dot3(high, low, wave_h[...], wave_l[...])
            for i in range(8):
                r = g * 8 + i
                value, slope = along[i * span : (i + 1) * span, :atoms], along[i * span : (i + 1) * span, atoms:]
                wy, dy = wy_ref[0, r : r + 1], wy_ref[1, r : r + 1]
                acc_ref[0] += value * wy
                acc_ref[1] += value * dy
                acc_ref[2] += slope * wy
        off = lax.broadcasted_iota(jnp.int32, (span, atoms), 0) + z_first - row(0).astype(jnp.int32)
        wz = dz = jnp.zeros((span, atoms), F32)
        for a in range(ORDER):
            wz = jnp.where(off == a, row(3 + a), wz)
            dz = jnp.where(off == a, row(7 + a), dz)
        total = lambda v: jnp.sum(v, axis=0, keepdims=True)
        out_ref[p] = jnp.concatenate(
            [total(acc_ref[0] * dz), total(acc_ref[1] * wz), total(acc_ref[2] * wz), jnp.zeros((5, atoms), F32)], axis=0)
        return carry

    lax.fori_loop(0, slabs, slab, 0)


def solve(moved, here, qm_table, kx_index, ky_index, points):
    rows, parts, z_local, lanes = moved.shape
    kx_local, block = kx_index.shape[0], ky_index.shape[0]
    half = points // 2
    atoms = qm_table.shape[2]
    k = np.arange(half)
    z = np.arange(points)
    angle = 2.0 * np.pi / points * ((k[:, None] * z[None, :]) % points)
    forward = np.concatenate([np.cos(angle), np.sin(angle)], axis=0)
    reach = points + 8
    backward = forward.T[np.arange(reach) % points]
    fh, fl = split_table(forward)
    bh, bl = split_table(backward)

    def parts_of(index):
        square, spline, _ = moduli(index, points)
        decay = jnp.exp(-(math.pi * math.pi / (SPLITTING * SPLITTING)) * square)
        return square, spline * decay * jnp.where(index == 0, 1.0, 2.0)

    z_sq, z_fac = parts_of(jnp.asarray(k, jnp.int32))
    x_sq, x_fac = parts_of(kx_index)
    y_sq, y_fac = parts_of(ky_index)

    def packed(y_part, x_part, combine):
        x_part = jnp.concatenate([x_part, x_part])
        full = combine(y_part[:, None], x_part[None, :]).reshape(block // 8, 8, 2 * kx_local)
        tail = full[:, :, lanes:].reshape(block // 8, 2, 4, lanes // 2).transpose(0, 2, 1, 3).reshape(block // 8, 4, lanes)
        return jnp.concatenate([full[:, :, :lanes], tail], axis=1).reshape(rows, lanes)

    col = packed(y_fac, x_fac, lambda a, b: a * b) * (1.0 / (math.pi * float(points) ** 3))
    sq = packed(y_sq, x_sq, lambda a, b: a + b)
    az = jnp.broadcast_to(z_fac[:, None], (half, lanes))
    sz = jnp.broadcast_to(z_sq[:, None], (half, lanes))
    kx_lane = jnp.concatenate([kx_index, kx_index, jnp.zeros((2 * LANES - 2 * kx_local,), jnp.int32)])
    turn = 2.0 * math.pi / points * (jnp.arange(ORDER, dtype=jnp.int32)[:, None] * kx_lane[None, :] % points).astype(F32)
    step = jnp.concatenate([jnp.cos(turn), jnp.sin(turn)], axis=0)
    step = jnp.broadcast_to(step[:, :, None], step.shape + (lanes,))
    vmem = pl.BlockSpec(memory_space=pltpu.VMEM)
    return pl.pallas_call(
        functools.partial(solve_kernel, points, kx_local, block),
        in_specs=[pl.BlockSpec(memory_space=pltpu.SMEM)] + [vmem] * 11,
        out_specs=vmem,
        out_shape=jax.ShapeDtypeStruct((qm_table.shape[0], 8, atoms), F32),
        scratch_shapes=[
            pltpu.VMEM((rows, reach, lanes), F32),
            pltpu.VMEM((2 * LANES, 2 * atoms), BF16),
            pltpu.VMEM((2 * LANES, 2 * atoms), BF16),
            pltpu.VMEM((2, block, atoms), F32),
            pltpu.VMEM((3, 32, atoms), F32),
        ],
        compiler_params=pltpu.CompilerParams(vmem_limit_bytes=VMEM_LIMIT),
        name="solve_interpolate",
    )(here, moved.reshape(rows, parts * z_local, lanes), fh, fl, bh, bl, az, sz, col, sq, step, qm_table)


def reduce_kernel(count_z, count_y, part_ref, out_ref, land_ref, send_sem, recv_sem):
    p = lax.axis_index("gz")
    y = lax.axis_index("gy")
    me = p * count_y + y
    total = count_z * count_y
    width = out_ref.shape[1]
    barrier = pltpu.get_barrier_semaphore()
    for d in range(1, total):
        other = lax.rem(me + d, total)
        pl.semaphore_signal(barrier, inc=1, device_id=(other // count_y, lax.rem(other, count_y)), device_id_type=MESH)
    pl.semaphore_wait(barrier, total - 1)
    for d in range(1, total):
        other = lax.rem(me + d, total)
        pltpu.make_async_remote_copy(
            src_ref=part_ref.at[other], dst_ref=land_ref.at[me], send_sem=send_sem, recv_sem=recv_sem,
            device_id=(other // count_y, lax.rem(other, count_y)), device_id_type=MESH).start()
    land_ref[me] = part_ref[me]
    pltpu.make_async_remote_copy(
        src_ref=land_ref.at[pl.ds(0, total - 1)], dst_ref=land_ref.at[pl.ds(0, total - 1)], send_sem=send_sem, recv_sem=recv_sem,
        device_id=(p, 1 - y), device_id_type=MESH).wait()
    out_ref[...] = jnp.sum(land_ref[...], axis=0)


def reduce_forces(partial, count_z, count_y):
    total, rows, width = partial.shape
    vmem = pl.BlockSpec(memory_space=pltpu.VMEM)
    return pl.pallas_call(
        functools.partial(reduce_kernel, count_z, count_y),
        in_specs=[vmem],
        out_specs=vmem,
        out_shape=jax.ShapeDtypeStruct((rows, width), F32),
        scratch_shapes=[pltpu.VMEM((total, rows, width), F32), pltpu.SemaphoreType.DMA, pltpu.SemaphoreType.DMA],
        compiler_params=pltpu.CompilerParams(collective_id=2, has_side_effects=True, vmem_limit_bytes=VMEM_LIMIT),
        name="reduce_forces",
    )(partial)


def fast_shards(spread_weights, spread_base, qm_base, qm_frac, qm_charge):
    points = GRID
    count_z = lax.axis_size("gz")
    count_y = lax.axis_size("gy")
    z_local, y_local = points // count_z, points // count_y
    kx_local = points // 2 // count_y
    block = points // count_z
    p = lax.axis_index("gz")
    q = lax.axis_index("gy")
    count = spread_weights.shape[1]
    qm_count = qm_base.shape[1]

    z_cell = spread_base[0] - p * z_local
    y_cell = spread_base[1] - q * y_local
    cells = jnp.stack([z_cell, y_cell, spread_base[2]]).astype(F32)
    table = jnp.concatenate(
        [spread_weights.reshape(ORDER * ORDER, ORDER, count).transpose(1, 0, 2).reshape(ORDER**3, count),
         cells, jnp.zeros((5, count), F32)], axis=0)
    own = order_by(y_cell, table)
    lower = cells - jnp.asarray([z_local, 0, 0], F32)[:, None]
    halo = order_by(y_cell + jnp.where(z_cell + ORDER > z_local, 0, y_local), table)
    halo = jnp.concatenate([halo[: ORDER**3], halo[ORDER**3 : ORDER**3 + 1] - z_local, halo[ORDER**3 + 1 :]], axis=0)
    qm = jnp.concatenate([qm_base.astype(F32), qm_frac, jnp.zeros((2, qm_count), F32)], axis=0)
    tab, qm_all = gather(own, halo, qm, count_z, count_y)

    lines = spread(tab, q * kx_local, kx_local, z_local, y_local, points)
    send = transform_rows(lines, jnp.stack([p // PLANE, p % PLANE]), y_local, points)
    moved = exchange(send)

    qm_all = qm_all.transpose(1, 0, 2).reshape(8, count_z, count_y * qm_count)
    w_z, d_z = spline_weights(qm_all[3])
    w_y, d_y = spline_weights(qm_all[4])
    w_x, d_x = spline_weights(qm_all[5])
    qm_table = jnp.concatenate([qm_all[:3], w_z, d_z, w_y, d_y, w_x, d_x, jnp.zeros((5,) + qm_all.shape[1:], F32)], axis=0)
    qm_table = qm_table.transpose(1, 0, 2)
    kx_index = q * kx_local + jnp.arange(kx_local, dtype=jnp.int32)
    ky_first = (p // 2) * block
    ky_index = ky_first + jnp.arange(block, dtype=jnp.int32)
    y_shift = jnp.where(p % 2 == 0, points, points - points // 4)
    here = jnp.stack([q * kx_local, ky_first, y_shift])
    partial = solve(moved, here, qm_table, kx_index, ky_index, points)
    partial = partial.reshape(count_z, 8, count_y, qm_count).transpose(0, 2, 1, 3).reshape(count_z * count_y, 8, qm_count)
    forces = reduce_forces(partial, count_z, count_y)
    return -qm_charge * forces[:3]


def quick(mesh):
    return mesh.shape["gz"] == RING * PLANE and mesh.shape["gy"] == 2


def solution(mesh):
    in_specs = (
        P(None, ("gz", "gy")),
        P(None, ("gz", "gy")),
        P(None, ("gz", "gy")),
        P(None, ("gz", "gy")),
        P(("gz", "gy")),
    )
    out_specs = P(None, ("gz", "gy"))
    body = fast_shards if quick(mesh) else shards
    return jax.shard_map(body, mesh=mesh, in_specs=in_specs, out_specs=out_specs, check_vma=False)
```

```python
import functools
import math

import jax
import jax.numpy as jnp
import numpy as np
from jax import lax
from jax.experimental import pallas as pl
from jax.experimental.pallas import tpu as pltpu
from jax.sharding import PartitionSpec as P

GRID = 384
ORDER = 4


SPLITTING = 0.8
HIGHEST = lax.Precision.HIGHEST
HIGH = lax.Precision.HIGH
GROUP = 64


def moduli(index, points):
    signed = jnp.where(index < points // 2, index, index - points).astype(jnp.float32) / points
    spline = 2.0 / 3.0 + jnp.cos(2.0 * math.pi / points * index.astype(jnp.float32)) / 3.0
    return (signed * signed, 1.0 / (spline * spline), index == points // 2)


def influence(first, second, third, points):
    sq_one, mod_one, edge_one = moduli(first, points)
    sq_two, mod_two, edge_two = moduli(second, points)
    sq_three, mod_three, edge_three = moduli(third, points)
    total = sq_one + sq_two + sq_three
    safe = jnp.where(total > 0.0, total, 1.0)
    value = (
        mod_one
        * mod_two
        * mod_three
        * jnp.exp(-(math.pi * math.pi / (SPLITTING * SPLITTING)) * total)
        / (math.pi * safe)
    )
    keep = (total > 0.0) & jnp.logical_not(edge_one | edge_two | edge_three)
    return jnp.where(keep, value, 0.0)


def spline_weights(frac):
    remain = 1.0 - frac
    square = frac * frac
    cubed = square * frac
    values = jnp.stack(
        [
            remain * remain * remain / 6.0,
            (3.0 * cubed - 6.0 * square + 4.0) / 6.0,
            (-3.0 * cubed + 3.0 * square + 3.0 * frac + 1.0) / 6.0,
            cubed / 6.0,
        ]
    )
    slopes = jnp.stack(
        [
            -0.5 * remain * remain,
            (3.0 * square - 4.0 * frac) / 2.0,
            (-3.0 * square + 2.0 * frac + 1.0) / 2.0,
            0.5 * square,
        ]
    )
    return (values, slopes)


def angle_tables(rows_in, cols_in, points):
    product = rows_in[:, None] * cols_in[None, :] % points
    angle = 2.0 * math.pi / points * product.astype(jnp.float32)
    return (jnp.cos(angle), jnp.sin(angle))


def line_tables(cells, values, slopes, extent):
    hits = (jnp.arange(extent, dtype=jnp.int32)[None, :, None] == cells[:, None, :]).astype(
        jnp.float32
    )
    return (jnp.sum(hits * values[:, None, :], axis=0), jnp.sum(hits * slopes[:, None, :], axis=0))


def spread_kernel(first_ref, count_ref, weights_ref, z_ref, y_ref, waves_ref, out_ref):
    half = pl.program_id(0)
    group = pl.program_id(1)

    @pl.when(group == 0)
    def _():
        out_ref[...] = jnp.zeros_like(out_ref)

    rows = out_ref.shape[1]
    weights = weights_ref[...]
    z_cell = z_ref[...]
    y_cell = y_ref[...]
    waves = waves_ref[...]
    high = waves.astype(jnp.bfloat16)
    low = (waves - high.astype(jnp.float32)).astype(jnp.bfloat16)
    first = first_ref[half, group]
    row_offset = lax.broadcasted_iota(jnp.int32, (rows, weights.shape[1]), 0) - y_cell

    def plane(step, carry):
        z = first + step
        offset = z - z_cell
        chosen = jnp.zeros((ORDER, weights.shape[1]), jnp.float32)
        for a in range(ORDER):
            chosen = jnp.where(offset == a, weights[a * ORDER : (a + 1) * ORDER], chosen)
        placed = jnp.zeros((rows, weights.shape[1]), jnp.float32)
        for b in range(ORDER):
            placed = jnp.where(row_offset == b, chosen[b : b + 1], placed)
        top = placed.astype(jnp.bfloat16)
        rest = (placed - top.astype(jnp.float32)).astype(jnp.bfloat16)
        total = jnp.dot(top, high, preferred_element_type=jnp.float32)
        total += jnp.dot(rest, high, preferred_element_type=jnp.float32)
        total += jnp.dot(top, low, preferred_element_type=jnp.float32)
        out_ref[z] += total
        return carry

    lax.fori_loop(0, count_ref[half, group], plane, 0)


def sort_by_plane(table, local_z):
    count = local_z.shape[0]
    order = jnp.arange(count, dtype=jnp.int32)
    before = (local_z[:, None] < local_z[None, :]) | (
        (local_z[:, None] == local_z[None, :]) & (order[:, None] < order[None, :])
    )
    rank = jnp.sum(before.astype(jnp.int32), axis=0)
    moves = (rank[:, None] == order[None, :]).astype(jnp.float32)
    return jnp.dot(table, moves, precision=HIGHEST)


def phases(cells, index, points):
    angle = (2.0 * math.pi / points) * (cells[..., None] * index % points).astype(jnp.float32)
    return (jnp.cos(angle), jnp.sin(angle))


def spread_lines(spread_weights, spread_base, z_first, y_first, z_extent, y_local, kx_index, points):
    count = spread_weights.shape[1]
    halves = lax.axis_size("gy")
    local = jnp.stack([spread_base[0] - z_first, spread_base[1] - y_first, spread_base[2]])
    table = jnp.concatenate([spread_weights, local.astype(jnp.float32)], axis=0)
    table = sort_by_plane(table, local[0])
    table = lax.all_gather(table, "gy")
    groups = count // GROUP
    width = ORDER * GROUP
    weights = table[:, : ORDER**3].reshape(halves, ORDER * ORDER, ORDER, groups, GROUP)
    weights = weights.transpose(0, 3, 1, 2, 4).reshape(halves, groups, ORDER * ORDER, width)
    cells = jnp.round(table[:, ORDER**3 :]).astype(jnp.int32).reshape(halves, 3, groups, GROUP)
    z_cell, y_cell, x_cell = cells[:, 0], cells[:, 1], cells[:, 2]
    first = jnp.min(z_cell, axis=-1)
    planes = jnp.max(z_cell, axis=-1) - first + ORDER
    z_wide = jnp.tile(z_cell, (1, 1, ORDER))[:, :, None, :]
    y_wide = jnp.tile(y_cell, (1, 1, ORDER))[:, :, None, :]
    cosine, sine = phases(x_cell, kx_index, points)
    step_cos, step_sin = phases(jnp.arange(ORDER, dtype=jnp.int32), kx_index, points)
    step_cos, step_sin = step_cos[:, None, :], step_sin[:, None, :]
    cosine, sine = cosine[:, :, None], sine[:, :, None]
    waves = jnp.concatenate(
        [cosine * step_cos - sine * step_sin, -(sine * step_cos + cosine * step_sin)], axis=-1
    ).reshape(halves, groups, width, -1)
    rows = -(-(y_local + ORDER - 1) // 8) * 8
    lanes = waves.shape[-1]
    per_group = lambda q, g, *_: (q, g, 0, 0)
    lines = pl.pallas_call(
        spread_kernel,
        grid_spec=pltpu.PrefetchScalarGridSpec(
            num_scalar_prefetch=2,
            grid=(halves, groups),
            in_specs=[
                pl.BlockSpec((None, None, ORDER * ORDER, width), per_group),
                pl.BlockSpec((None, None, 1, width), per_group),
                pl.BlockSpec((None, None, 1, width), per_group),
                pl.BlockSpec((None, None, width, lanes), per_group),
            ],
            out_specs=pl.BlockSpec((z_extent, None, rows, lanes), lambda q, g, *_: (0, q, 0, 0)),
        ),
        out_shape=jax.ShapeDtypeStruct((z_extent, halves, rows, lanes), jnp.float32),
        compiler_params=pltpu.CompilerParams(dimension_semantics=("arbitrary", "arbitrary")),
    )(first, planes, weights, z_wide, y_wide, waves)
    return lines, rows


def line_waves(cell, values, slopes, index, points):
    cosine, sine = phases(cell, index, points)
    step_cos, step_sin = phases(jnp.arange(ORDER, dtype=jnp.int32), index, points)
    found = []
    for table in (values, slopes):
        real = sum(table[c][..., None] * step_cos[c] for c in range(ORDER))
        imag = sum(table[c][..., None] * step_sin[c] for c in range(ORDER))
        found.append((cosine * real - sine * imag, cosine * imag + sine * real))
    return found


def slab_forces(lines, base, frac, z_first, y_index, x_index, points):
    z_extent, ky_local, _, kx_local = lines.shape
    shifts = jnp.arange(ORDER, dtype=jnp.int32)[:, None]
    w_z, d_z = spline_weights(frac[0])
    w_y, d_y = spline_weights(frac[1])
    w_x, d_x = spline_weights(frac[2])
    plane_w, plane_d = line_tables(base[0][None, :] - z_first + shifts, w_z, d_z, z_extent)
    (wy_re, wy_im), (dy_re, dy_im) = line_waves(base[1], w_y, d_y, y_index, points)
    (wx_re, wx_im), (dx_re, dx_im) = line_waves(base[2], w_x, d_x, x_index, points)
    join = lambda a, b: jnp.concatenate([a, b], axis=1)
    waves = jnp.stack([join(wx_re, -wx_im), join(wx_im, wx_re), join(dx_re, -dx_im), join(dx_im, dx_re)])
    count = base.shape[1]
    along = jnp.einsum(
        "mk,nk->mn",
        lines.reshape(z_extent * ky_local, 2 * kx_local),
        waves.reshape(4 * count, 2 * kx_local),
        precision=HIGH,
    ).reshape(z_extent, ky_local, 4, count)
    wy_re, wy_im, dy_re, dy_im = wy_re.T, wy_im.T, dy_re.T, dy_im.T
    plain = jnp.sum(along[:, :, 0] * wy_re - along[:, :, 1] * wy_im, axis=1)
    tilted = jnp.sum(along[:, :, 0] * dy_re - along[:, :, 1] * dy_im, axis=1)
    sloped = jnp.sum(along[:, :, 2] * wy_re - along[:, :, 3] * wy_im, axis=1)
    return jnp.stack(
        [
            jnp.sum(plain * plane_d, axis=0),
            jnp.sum(tilted * plane_w, axis=0),
            jnp.sum(sloped * plane_w, axis=0),
        ]
    )


def shards(spread_weights, spread_base, qm_base, qm_frac, qm_charge):
    points = GRID
    margin = ORDER - 1
    count_z = lax.axis_size("gz")
    count_y = lax.axis_size("gy")
    z_local = points // count_z
    y_local = points // count_y
    z_extent = z_local + margin
    kx_count = points // 2
    kx_local = kx_count // count_y
    ky_local = points // count_z
    z_first = lax.axis_index("gz") * z_local
    y_first = lax.axis_index("gy") * y_local
    ky_index = lax.axis_index("gz") * ky_local + jnp.arange(ky_local, dtype=jnp.int32)
    kx_index = lax.axis_index("gy") * kx_local + jnp.arange(kx_local, dtype=jnp.int32)
    positions = jnp.arange(points, dtype=jnp.int32)
    all_base = lax.all_gather(qm_base, ("gz", "gy"), axis=1, tiled=True)
    all_frac = lax.all_gather(qm_frac, ("gz", "gy"), axis=1, tiled=True)

    lines, rows = spread_lines(
        spread_weights, spread_base, z_first, y_first, z_extent, y_local, kx_index, points
    )
    row_cells = (
        jnp.arange(count_y, dtype=jnp.int32)[:, None] * y_local
        + jnp.arange(rows, dtype=jnp.int32)[None, :]
    ).reshape(-1) % points
    tables = jnp.concatenate(angle_tables(positions, row_cells, points), axis=0)
    lines = lines.reshape(z_extent, count_y * rows, 2 * kx_local)
    both = jnp.einsum("yr,zrk->zyk", tables, lines, precision=HIGH)
    with_cos, with_sin = both[:, :points], both[:, points:]
    packed = jnp.stack(
        [
            with_cos[:, :, :kx_local] + with_sin[:, :, kx_local:],
            with_cos[:, :, kx_local:] - with_sin[:, :, :kx_local],
        ],
        axis=1,
    )
    packed = packed.reshape(z_extent, 2, count_z, ky_local, kx_local).transpose(2, 0, 1, 3, 4)
    packed = packed.reshape(count_z, z_extent * 2 * ky_local * kx_local)
    moved = lax.all_to_all(packed, "gz", split_axis=0, concat_axis=0, tiled=True)

    z_cells = (
        jnp.arange(count_z, dtype=jnp.int32)[:, None] * z_local
        + jnp.arange(z_extent, dtype=jnp.int32)[None, :]
    ).reshape(-1) % points
    cells = ky_local * kx_local
    moved = moved.reshape(count_z * z_extent, 2 * cells)
    tables = jnp.concatenate(angle_tables(positions, z_cells, points), axis=0)
    both = jnp.dot(tables, moved, precision=HIGH).reshape(2, points, 2, ky_local, kx_local)
    green = influence(
        positions[:, None, None], ky_index[None, :, None], kx_index[None, None, :], points
    )
    kx_weight = jnp.where(kx_index == 0, 1.0, 2.0).astype(jnp.float32)
    green = green * (kx_weight * (1.0 / float(points * points * points)))
    spectrum = jnp.stack(
        [(both[0, :, 0] + both[1, :, 1]) * green, (both[0, :, 1] - both[1, :, 0]) * green], axis=1
    ).reshape(points, 2 * cells)
    back = jnp.concatenate(angle_tables(z_cells, positions, points), axis=0)
    both = jnp.dot(back, spectrum, precision=HIGH)
    both = both.reshape(2, count_z, z_extent, 2, ky_local, kx_local)
    lines = jnp.stack(
        [both[0, :, :, 0] - both[1, :, :, 1], both[0, :, :, 1] + both[1, :, :, 0]], axis=3
    )

    def one_slab(args):
        slab, base, frac, start = args
        return slab_forces(slab, base, frac, start, ky_index, kx_index, points)

    slab_base = all_base.reshape(3, count_z, -1).transpose(1, 0, 2)
    slab_frac = all_frac.reshape(3, count_z, -1).transpose(1, 0, 2)
    starts = jnp.arange(count_z, dtype=jnp.int32) * z_local
    partial = lax.map(one_slab, (lines, slab_base, slab_frac, starts))
    forces = lax.psum_scatter(
        partial.transpose(1, 0, 2).reshape(3, -1), ("gz", "gy"), scatter_dimension=1, tiled=True
    )
    return -qm_charge * forces


MESH = pl.DeviceIdType.MESH
RING = 4
PLANE = 4
LANES = 128
F32 = jnp.float32
BF16 = jnp.bfloat16
VMEM_LIMIT = 62 * 2**20


def split_table(table):
    high = table.astype(np.float32).astype(BF16)
    low = (table - high.astype(np.float64)).astype(np.float32).astype(BF16)
    return jnp.asarray(high), jnp.asarray(low)


def split(value):
    high = value.astype(BF16)
    return high, (value - high.astype(F32)).astype(BF16)


def dot3(a_high, a_low, b_high, b_low):
    total = jnp.dot(a_high, b_high, preferred_element_type=F32)
    total += jnp.dot(a_low, b_high, preferred_element_type=F32)
    return total + jnp.dot(a_high, b_low, preferred_element_type=F32)


def trig(units, points):
    rest = units - points * jnp.floor((units + 0.5) * (1.0 / points))
    quarter = points // 4
    turn = jnp.floor((rest + quarter / 2) * (1.0 / quarter))
    angle = (rest - quarter * turn) * (2.0 * math.pi / points)
    square = angle * angle
    sine = angle * (1.0 + square * (-1.0 / 6 + square * (1.0 / 120 + square * (-1.0 / 5040 + square / 362880))))
    cosine = 1.0 + square * (-0.5 + square * (1.0 / 24 + square * (-1.0 / 720 + square * (1.0 / 40320))))
    odd = (turn == 1.0) | (turn == 3.0)
    first = jnp.where(odd, sine, cosine)
    second = jnp.where(odd, cosine, sine)
    first = jnp.where((turn == 1.0) | (turn == 2.0), -first, first)
    second = jnp.where((turn == 2.0) | (turn == 3.0), -second, second)
    return first, second


def order_by(key, table):
    count = key.shape[0]
    order = jnp.arange(count, dtype=jnp.int32)
    before = (key[:, None] < key[None, :]) | ((key[:, None] == key[None, :]) & (order[:, None] < order[None, :]))
    rank = jnp.sum(before.astype(jnp.int32), axis=0)
    moves = (rank[:, None] == order[None, :]).astype(F32)
    return jnp.dot(table, moves, precision=HIGHEST)


def gather_kernel(own_ref, qm_ref, tab_ref, all_ref, zs, zr, xs, xr, ys, yr, fs, fr, gs, gr, qm_send, qm_recv):
    p = lax.axis_index("gz")
    y = lax.axis_index("gy")
    me = p * 2 + y
    total = RING * PLANE * 2
    ring, spot = p // PLANE, lax.rem(p, PLANE)
    x, core = spot // 2, lax.rem(spot, 2)
    barrier = pltpu.get_barrier_semaphore()
    for d in range(1, total):
        other = lax.rem(me + d, total)
        pl.semaphore_signal(barrier, inc=1, device_id=(other // 2, lax.rem(other, 2)), device_id_type=MESH)
    pl.semaphore_wait(barrier, total - 1)

    def place(z, xx, yy):
        return (z * 2 + xx) * 2 + yy

    def copy(src, dst, s, r, device):
        return pltpu.make_async_remote_copy(src_ref=src, dst_ref=dst, send_sem=s, recv_sem=r, device_id=device, device_id_type=MESH)

    above = (p + PLANE, y)
    below = (p - PLANE, y)
    aside = (ring * PLANE + (1 - x) * 2 + core, y)
    over = (p, 1 - y)
    cut = tab_ref.shape[1] // 16 * 8
    tab_ref[place(ring, x, y)] = own_ref[...]
    for d in range(1, total):
        other = lax.rem(me + d, total)
        copy(qm_ref, all_ref.at[me], qm_send, qm_recv, (other // 2, lax.rem(other, 2))).start()
    all_ref[me] = qm_ref[...]
    lower = (RING - 1 - ring) // 2
    near = ring + 1 - 2 * lax.rem(ring, 2)
    order = [ring, near, 1 + lower, (RING - 1) * lower]

    def along(z, i):
        src = own_ref if i == 0 else tab_ref.at[place(z, x, y)]
        dst = tab_ref.at[place(z, x, y)]
        return copy(src, dst, zs.at[0, z], zr.at[z], above), copy(src, dst, zs.at[1, z], zr.at[z], below)

    def flat(z, i):
        src = own_ref if i == 0 else tab_ref.at[place(z, x, y)]
        dst = tab_ref.at[place(z, x, y)]
        return copy(src, dst, xs.at[z], xr.at[z], aside), copy(src, dst, ys.at[z], yr.at[z], over)

    def turn(z):
        first = tab_ref.at[place(z, 1 - x, y), pl.ds(0, cut)]
        second = tab_ref.at[place(z, x, 1 - y), pl.ds(cut, tab_ref.shape[1] - cut)]
        return copy(first, first, fs.at[z], fr.at[z], over), copy(second, second, gs.at[z], gr.at[z], aside)

    def corner(z):
        first = tab_ref.at[place(z, 1 - x, 1 - y), pl.ds(0, cut)]
        second = tab_ref.at[place(z, 1 - x, 1 - y), pl.ds(cut, tab_ref.shape[1] - cut)]
        return copy(first, first, fs.at[z], fr.at[z], over), copy(second, second, gs.at[z], gr.at[z], aside)

    def upward(z):
        return (z <= ring) & (ring < RING - 1)

    def downward(z):
        return (z >= ring) & (ring > 0)

    def relay(z):
        mine = tab_ref.at[place(z, 1 - x, y)]
        theirs = tab_ref.at[place(z, x, 1 - y)]
        copy(mine, mine, xs.at[z], xr.at[z], aside).wait_recv()
        copy(theirs, theirs, ys.at[z], yr.at[z], over).wait_recv()
        for c in turn(z):
            c.start()

    for i, z in enumerate(order):
        up, down = along(z, i)
        if i:
            up.wait_recv()

        @pl.when(upward(z))
        def _():
            up.start()

        @pl.when(downward(z))
        def _():
            down.start()

        for c in flat(z, i):
            c.start()
        if i:
            relay(order[i - 1])
    relay(order[-1])
    for i, z in enumerate(order):
        for c in corner(z):
            c.wait_recv()
    for i, z in enumerate(order):
        up, down = along(z, i)

        @pl.when(upward(z))
        def _():
            up.wait_send()

        @pl.when(downward(z))
        def _():
            down.wait_send()

        for c in flat(z, i) + turn(z):
            c.wait_send()
    rest = all_ref.at[pl.ds(0, total - 1)]
    copy(rest, rest, qm_send, qm_recv, over).wait()


def gather(own, qm):
    vmem = pl.BlockSpec(memory_space=pltpu.VMEM)
    ring = pltpu.SemaphoreType.DMA((RING,))
    single = pltpu.SemaphoreType.DMA
    return pl.pallas_call(
        gather_kernel,
        out_shape=(
            jax.ShapeDtypeStruct((RING * 4,) + own.shape, F32),
            jax.ShapeDtypeStruct((RING * PLANE * 2,) + qm.shape, F32),
        ),
        in_specs=[vmem] * 2,
        out_specs=(vmem, vmem),
        scratch_shapes=[pltpu.SemaphoreType.DMA((2, RING))] + [ring] * 9 + [single, single],
        compiler_params=pltpu.CompilerParams(collective_id=0, has_side_effects=True, vmem_limit_bytes=VMEM_LIMIT),
        name="gather_atoms",
    )(own, qm)


Z_STEP = 6
BLOCK = 256


def lines_kernel(points, kx_local, z_used, kx_ref, first_ref, count_ref, tab_ref, th_ref, tl_ref, out_ref, grid_ref):
    slab, half, block = pl.program_id(0), pl.program_id(1), pl.program_id(2)
    blocks = pl.num_programs(2)
    modes = 2 * kx_local
    part = LANES // 2
    rows = ORDER * ORDER

    @pl.when((half == 0) & (block == 0))
    def _():
        grid_ref[...] = jnp.zeros_like(grid_ref)

    lane = lax.broadcasted_iota(jnp.int32, (1, LANES), 1)
    mode = lax.broadcasted_iota(jnp.int32, (modes, LANES), 0)
    sine = mode >= kx_local
    kx = (kx_ref[0] + jnp.where(sine, mode - kx_local, mode)).astype(F32)
    shift = jnp.where(sine, points - points // 4, points).astype(F32)
    steps = [trig(kx * float(c), points) for c in range(ORDER)]
    wide = lax.broadcasted_iota(jnp.int32, (1, 2 * LANES), 1)
    y_shift = wide // part
    y_rows = lax.broadcasted_iota(jnp.int32, (2 * LANES, 2 * LANES), 0)
    z_rows = lax.broadcasted_iota(jnp.int32, (8, 2 * LANES), 0)
    base = ((slab * 2 + half) * blocks + block) * (BLOCK // part)
    most = count_ref[base]
    for g in range(1, BLOCK // part):
        most = jnp.maximum(most, count_ref[base + g])

    def step(it, carry):
        for g in range(BLOCK // part):
            tab = tab_ref[:, (g // 2) * LANES : (g // 2 + 1) * LANES]

            def pair(even, odd):
                if g % 2 == 0:
                    return jnp.where(lane < part, even, pltpu.roll(odd, part, 1))
                return jnp.where(lane < part, pltpu.roll(even, part, 1), odd)

            weights = jnp.concatenate(
                [pair(tab[0:rows], tab[rows : 2 * rows]), pair(tab[2 * rows : 3 * rows], tab[3 * rows : 4 * rows])], axis=1)
            spots = tab[4 * rows : 4 * rows + 8]
            spots = pair(spots, spots)
            twice = jnp.concatenate([spots, spots], axis=1).astype(jnp.int32)
            z_first = first_ref[base + g] + it * Z_STEP
            live = it < count_ref[base + g]
            off = z_rows + jnp.where(live, z_first, 4 * points) - twice[0:1]
            z_first = jnp.minimum(z_first, z_used - 1)
            cosine, sinus = trig(kx * spots[2:3] + shift, points)
            waves, picks = [], []
            for c in range(ORDER):
                wave = cosine * steps[c][0] - sinus * steps[c][1] if c else cosine
                waves.append(jnp.concatenate([wave, wave], axis=1))
                pick = jnp.zeros((8, 2 * LANES), F32)
                for a in range(ORDER):
                    pick = jnp.where(off == a, weights[a * ORDER + c : a * ORDER + c + 1], pick)
                picks.append(pick)
            pieces = []
            for z in range(Z_STEP):
                value = picks[0][z : z + 1] * waves[0]
                for c in range(1, ORDER):
                    value += picks[c][z : z + 1] * waves[c]
                pieces.append(value)
            high, low = split(jnp.concatenate(pieces, axis=0))
            hits = jnp.where(y_rows == twice[1:2] + y_shift, 1.0, 0.0).astype(BF16)
            across = (((1,), (1,)), ((), ()))
            total = lax.dot_general(high, hits, across, preferred_element_type=F32)
            total += lax.dot_general(low, hits, across, preferred_element_type=F32)
            grid_ref[half, pl.ds(pl.multiple_of(z_first * modes, 8), Z_STEP * modes), :] += total
        return carry

    lax.fori_loop(0, most, step, 0)

    @pl.when((half == 1) & (block == blocks - 1))
    def _():
        cuts = 3
        size = z_used * modes // cuts

        def chunk(i, carry):
            at = pl.multiple_of(i * size, 8)
            total = None
            for h in range(2):
                high, low = split(grid_ref[h, pl.ds(at, size), :])
                found = dot3(high, low, th_ref[h], tl_ref[h])
                total = found if total is None else total + found
            for t in range(4):
                out_ref[t // 2, t % 2, pl.ds(at, size), :] = total[:, t * LANES : (t + 1) * LANES]
            return carry

        lax.fori_loop(0, cuts, chunk, 0)


def spread(tab, kx_first, kx_local, z_local, y_local, points):
    tables, rows, count = tab.shape
    slabs = tables // 2
    part = LANES // 2
    z_used = z_local + ORDER - 1
    modes = 2 * kx_local
    z_cell = jnp.round(tab[:, 4 * ORDER * ORDER]).astype(jnp.int32).reshape(tables, count // part, part)
    first = jnp.min(z_cell, axis=-1)
    counts = (jnp.max(z_cell, axis=-1) - first + ORDER + Z_STEP - 1) // Z_STEP
    k = np.arange(points // 2)
    cell = (np.arange(2)[:, None] * y_local + np.arange(2 * LANES)[None, :]) % points
    angle = 2.0 * np.pi / points * ((cell[:, :, None] * k) % points)
    table = np.zeros((2, 2 * LANES, 2, 2 * LANES))
    table[:, :, 0, : points // 2] = np.cos(angle)
    table[:, :, 1, : points // 2] = np.sin(angle)
    th, tl = split_table(table.reshape(2, 2 * LANES, 4 * LANES))
    whole = lambda s, h, b, *_: (0, 0, 0)
    return pl.pallas_call(
        functools.partial(lines_kernel, points, kx_local, z_used),
        grid_spec=pltpu.PrefetchScalarGridSpec(
            num_scalar_prefetch=3,
            grid=(slabs, 2, count // BLOCK),
            in_specs=[
                pl.BlockSpec((None, rows, BLOCK), lambda s, h, b, *_: (s * 2 + h, 0, b)),
                pl.BlockSpec(th.shape, whole),
                pl.BlockSpec(tl.shape, whole),
            ],
            out_specs=pl.BlockSpec((2, 2, None, z_used * modes, LANES), lambda s, h, b, *_: (0, 0, s, 0, 0)),
            scratch_shapes=[pltpu.VMEM((2, (z_used + Z_STEP - 1) * modes, 2 * LANES), F32)],
        ),
        out_shape=jax.ShapeDtypeStruct((2, 2, slabs, z_used * modes, LANES), F32),
        compiler_params=pltpu.CompilerParams(dimension_semantics=("arbitrary",) * 3, vmem_limit_bytes=VMEM_LIMIT),
        name="spread_lines",
    )(kx_first.reshape(1), first.reshape(-1), counts.reshape(-1), tab, th, tl)


def swap_kernel(lines_ref, out_ref, send_sem, recv_sem):
    p = lax.axis_index("gz")
    y = lax.axis_index("gy")
    core = lax.rem(p, 2)
    other = p + 1 - 2 * core
    barrier = pltpu.get_barrier_semaphore()
    pl.semaphore_signal(barrier, inc=1, device_id=(other, y), device_id_type=MESH)
    pl.semaphore_wait(barrier, 1)
    copy = pltpu.make_async_remote_copy(
        src_ref=lines_ref.at[1 - core], dst_ref=out_ref.at[:, core], send_sem=send_sem, recv_sem=recv_sem,
        device_id=(other, y), device_id_type=MESH)
    copy.start()

    def keep(i, carry):
        for t in range(2):
            out_ref[t, core, i] = lines_ref[core, t, i]
        return carry

    lax.fori_loop(0, lines_ref.shape[2], keep, 0)
    copy.wait()


def swap(lines):
    types, tiles, slabs, deep, lanes = lines.shape
    vmem = pl.BlockSpec(memory_space=pltpu.VMEM)
    out = pl.pallas_call(
        swap_kernel,
        in_specs=[vmem],
        out_specs=vmem,
        out_shape=jax.ShapeDtypeStruct((tiles, 2, slabs, deep, lanes), F32),
        scratch_shapes=[pltpu.SemaphoreType.DMA, pltpu.SemaphoreType.DMA],
        compiler_params=pltpu.CompilerParams(collective_id=1, has_side_effects=True, vmem_limit_bytes=VMEM_LIMIT),
        name="swap_modes",
    )(lines)
    return out.reshape(tiles, 2 * slabs * deep, lanes)


def solve_kernel(points, kx_local, here_ref, x_ref, fh_ref, fl_ref, bh_ref, bl_ref, az_ref, sz_ref, col_ref, sq_ref, step_ref, qm_ref, out_ref, pot_ref, wave_h, wave_l, wx_ref, acc_ref):
    modes = 2 * kx_local
    deep = x_ref.shape[1] // modes
    half = points // 2
    slabs = qm_ref.shape[0]
    z_local = points // slabs
    atoms = qm_ref.shape[2]
    kx_first, y_shift = here_ref[0], here_ref[1]

    def convolve(m, carry):
        data = jnp.concatenate([x_ref[t, pl.ds(m, deep, stride=modes), :] for t in range(2)], axis=1)
        high, low = split(data)
        coef = dot3(fh_ref[...], fl_ref[...], high, low)
        total = sz_ref[...] + sq_ref[pl.ds(m, 1), :]
        keep = total > 0.0
        value = az_ref[...] * col_ref[pl.ds(m, 1), :] / jnp.where(keep, total, 1.0)
        green = jnp.where(keep, value, 0.0)
        high, low = split(coef * jnp.concatenate([green, green], axis=0))
        pot_ref[m] = dot3(bh_ref[...], bl_ref[...], high, low)
        return carry

    lax.fori_loop(0, modes, convolve, 0)
    span = 4 * 8
    wave_h[half:] = jnp.zeros((2 * LANES - half, 2 * atoms), BF16)
    wave_l[half:] = jnp.zeros((2 * LANES - half, 2 * atoms), BF16)
    ky = lax.broadcasted_iota(jnp.int32, (half, atoms), 0).astype(F32)
    mode = lax.broadcasted_iota(jnp.int32, (modes, atoms), 0)
    sine = mode >= kx_local
    kx = (kx_first + jnp.where(sine, mode - kx_local, mode)).astype(F32)
    x_shift = jnp.where(sine, points - points // 4, points).astype(F32)

    def slab(p, carry):
        qm = qm_ref[p]
        row = lambda i: qm[i : i + 1]
        cosine, sinus = trig(ky * row(1) + y_shift.astype(F32), points)
        for k, at in ((0, 11), (1, 15)):
            real = imag = None
            for c in range(ORDER):
                sc = jnp.concatenate([step_ref[c]] * (atoms // LANES), axis=1)
                ss = jnp.concatenate([step_ref[ORDER + c]] * (atoms // LANES), axis=1)
                real = row(at + c) * sc if real is None else real + row(at + c) * sc
                imag = row(at + c) * ss if imag is None else imag + row(at + c) * ss
            high, low = split(cosine * real - sinus * imag)
            wave_h[0:half, k * atoms : (k + 1) * atoms] = high
            wave_l[0:half, k * atoms : (k + 1) * atoms] = low
        plain_x = slope_x = jnp.zeros((modes, atoms), F32)
        for c in range(ORDER):
            wave, _ = trig(kx * (row(2) + float(c)) + x_shift, points)
            plain_x += row(19 + c) * wave
            slope_x += row(23 + c) * wave
        wx_ref[0] = plain_x
        wx_ref[1] = slope_x
        z_first = pl.multiple_of(p * z_local, 8)
        acc_ref[...] = jnp.zeros_like(acc_ref)
        for g in range(modes // 8):
            tiles = [pot_ref[g * 8 + i, pl.ds(z_first, span), :] for i in range(8)]
            high, low = split(jnp.concatenate(tiles, axis=0))
            along = dot3(high, low, wave_h[...], wave_l[...])
            for i in range(8):
                r = g * 8 + i
                value, slope = along[i * span : (i + 1) * span, :atoms], along[i * span : (i + 1) * span, atoms:]
                wx, dx = wx_ref[0, r : r + 1], wx_ref[1, r : r + 1]
                acc_ref[0] += value * wx
                acc_ref[1] += slope * wx
                acc_ref[2] += value * dx
        off = lax.broadcasted_iota(jnp.int32, (span, atoms), 0) + z_first - row(0).astype(jnp.int32)
        wz = dz = jnp.zeros((span, atoms), F32)
        for a in range(ORDER):
            wz = jnp.where(off == a, row(3 + a), wz)
            dz = jnp.where(off == a, row(7 + a), dz)
        total = lambda v: jnp.sum(v, axis=0, keepdims=True)
        out_ref[p] = jnp.concatenate(
            [total(acc_ref[0] * dz), total(acc_ref[1] * wz), total(acc_ref[2] * wz), jnp.zeros((5, atoms), F32)], axis=0)
        return carry

    lax.fori_loop(0, slabs, slab, 0)


def solve(lines, here, qm_table, kx_index, points):
    tiles, deep, lanes = lines.shape
    kx_local = kx_index.shape[0]
    modes = 2 * kx_local
    half = points // 2
    slabs, _, atoms = qm_table.shape
    z_local = points // slabs
    z_used = z_local + ORDER - 1
    k = np.arange(half)

    def waves(z):
        angle = 2.0 * np.pi / points * ((k[:, None] * z[None, :]) % points)
        return np.concatenate([np.cos(angle), np.sin(angle)], axis=0)

    core, pair, plane = np.meshgrid(np.arange(2), np.arange(slabs // 2), np.arange(z_used), indexing="ij")
    fh, fl = split_table(waves((((pair * 2 + core) * z_local + plane) % points).reshape(-1)))
    reach = points + 8
    bh, bl = split_table(waves(np.arange(reach) % points).T)

    def parts_of(index):
        square, spline, _ = moduli(index, points)
        decay = jnp.exp(-(math.pi * math.pi / (SPLITTING * SPLITTING)) * square)
        return square, spline * decay * jnp.where(index == 0, 1.0, 2.0)

    z_sq, z_fac = parts_of(jnp.asarray(k, jnp.int32))
    x_sq, x_fac = parts_of(jnp.concatenate([kx_index, kx_index]))
    pad = (0, 2 * lanes - half)
    y_sq, y_fac = jnp.pad(z_sq, pad), jnp.pad(z_fac, pad)
    col = x_fac[:, None] * y_fac[None, :] * (1.0 / (math.pi * float(points) ** 3))
    sq = x_sq[:, None] + y_sq[None, :]
    az = jnp.broadcast_to(z_fac[:, None], (half, 2 * lanes))
    sz = jnp.broadcast_to(z_sq[:, None], (half, 2 * lanes))
    turn = 2.0 * np.pi / points * (np.arange(ORDER)[:, None] * k[None, :] % points)
    step = np.concatenate([np.cos(turn), np.sin(turn)], axis=0)
    step = jnp.broadcast_to(jnp.asarray(step[:, :, None], F32), step.shape + (lanes,))
    vmem = pl.BlockSpec(memory_space=pltpu.VMEM)
    return pl.pallas_call(
        functools.partial(solve_kernel, points, kx_local),
        in_specs=[pl.BlockSpec(memory_space=pltpu.SMEM)] + [vmem] * 11,
        out_specs=vmem,
        out_shape=jax.ShapeDtypeStruct((slabs, 8, atoms), F32),
        scratch_shapes=[
            pltpu.VMEM((modes, reach, 2 * lanes), F32),
            pltpu.VMEM((2 * lanes, 2 * atoms), BF16),
            pltpu.VMEM((2 * lanes, 2 * atoms), BF16),
            pltpu.VMEM((2, modes, atoms), F32),
            pltpu.VMEM((3, 32, atoms), F32),
        ],
        compiler_params=pltpu.CompilerParams(vmem_limit_bytes=VMEM_LIMIT),
        name="solve_interpolate",
    )(here, lines, fh, fl, bh, bl, az, sz, col, sq, step, qm_table)


def reduce_kernel(count_z, count_y, part_ref, out_ref, land_ref, send_sem, recv_sem):
    p = lax.axis_index("gz")
    y = lax.axis_index("gy")
    me = p * count_y + y
    total = count_z * count_y
    width = out_ref.shape[1]
    barrier = pltpu.get_barrier_semaphore()
    for d in range(1, total):
        other = lax.rem(me + d, total)
        pl.semaphore_signal(barrier, inc=1, device_id=(other // count_y, lax.rem(other, count_y)), device_id_type=MESH)
    pl.semaphore_wait(barrier, total - 1)
    for d in range(1, total):
        other = lax.rem(me + d, total)
        pltpu.make_async_remote_copy(
            src_ref=part_ref.at[other], dst_ref=land_ref.at[me], send_sem=send_sem, recv_sem=recv_sem,
            device_id=(other // count_y, lax.rem(other, count_y)), device_id_type=MESH).start()
    land_ref[me] = part_ref[me]
    pltpu.make_async_remote_copy(
        src_ref=land_ref.at[pl.ds(0, total - 1)], dst_ref=land_ref.at[pl.ds(0, total - 1)], send_sem=send_sem, recv_sem=recv_sem,
        device_id=(p, 1 - y), device_id_type=MESH).wait()
    out_ref[...] = jnp.sum(land_ref[...], axis=0)


def reduce_forces(partial, count_z, count_y):
    total, rows, width = partial.shape
    vmem = pl.BlockSpec(memory_space=pltpu.VMEM)
    return pl.pallas_call(
        functools.partial(reduce_kernel, count_z, count_y),
        in_specs=[vmem],
        out_specs=vmem,
        out_shape=jax.ShapeDtypeStruct((rows, width), F32),
        scratch_shapes=[pltpu.VMEM((total, rows, width), F32), pltpu.SemaphoreType.DMA, pltpu.SemaphoreType.DMA],
        compiler_params=pltpu.CompilerParams(collective_id=2, has_side_effects=True, vmem_limit_bytes=VMEM_LIMIT),
        name="reduce_forces",
    )(partial)


def fast_shards(spread_weights, spread_base, qm_base, qm_frac, qm_charge):
    points = GRID
    count_z = lax.axis_size("gz")
    count_y = lax.axis_size("gy")
    z_local, y_local = points // count_z, points // count_y
    kx_local = points // (RING * PLANE * 2)
    p = lax.axis_index("gz")
    q = lax.axis_index("gy")
    count = spread_weights.shape[1]
    qm_count = qm_base.shape[1]

    z_cell = spread_base[0] - p * z_local
    y_cell = spread_base[1] - q * y_local
    cells = jnp.stack([z_cell, y_cell, spread_base[2]]).astype(F32)
    table = jnp.concatenate(
        [spread_weights.reshape(ORDER, ORDER, ORDER, count).transpose(1, 0, 2, 3).reshape(ORDER**3, count),
         cells, jnp.zeros((5, count), F32)], axis=0)
    own = order_by(z_cell, table)
    qm = jnp.concatenate([qm_base.astype(F32), qm_frac, jnp.zeros((2, qm_count), F32)], axis=0)
    tab, qm_all = gather(own, qm)

    kx_first = ((p // 2) * count_y + q) * kx_local
    lines = spread(tab, kx_first, kx_local, z_local, y_local, points)
    lines = swap(lines)

    qm_all = qm_all.transpose(1, 0, 2).reshape(8, count_z, count_y * qm_count)
    w_z, d_z = spline_weights(qm_all[3])
    w_y, d_y = spline_weights(qm_all[4])
    w_x, d_x = spline_weights(qm_all[5])
    qm_table = jnp.concatenate([qm_all[:3], w_z, d_z, w_y, d_y, w_x, d_x, jnp.zeros((5,) + qm_all.shape[1:], F32)], axis=0)
    qm_table = qm_table.transpose(1, 0, 2)
    kx_index = kx_first + jnp.arange(kx_local, dtype=jnp.int32)
    y_shift = jnp.where(p % 2 == 0, points, points - points // 4)
    here = jnp.stack([kx_first, y_shift])
    partial = solve(lines, here, qm_table, kx_index, points)
    partial = partial.reshape(count_z, 8, count_y, qm_count).transpose(0, 2, 1, 3).reshape(count_z * count_y, 8, qm_count)
    forces = reduce_forces(partial, count_z, count_y)
    return -qm_charge * forces[:3]


def quick(mesh):
    return mesh.shape["gz"] == RING * PLANE and mesh.shape["gy"] == 2


def solution(mesh):
    in_specs = (
        P(None, ("gz", "gy")),
        P(None, ("gz", "gy")),
        P(None, ("gz", "gy")),
        P(None, ("gz", "gy")),
        P(("gz", "gy")),
    )
    out_specs = P(None, ("gz", "gy"))
    body = fast_shards if quick(mesh) else shards
    return jax.shard_map(body, mesh=mesh, in_specs=in_specs, out_specs=out_specs, check_vma=False)
```

```python
import functools
import math

import jax
import jax.numpy as jnp
import numpy as np
from jax import lax
from jax.experimental import pallas as pl
from jax.experimental.pallas import tpu as pltpu
from jax.sharding import PartitionSpec as P

GRID = 384
ORDER = 4


SPLITTING = 0.8
HIGHEST = lax.Precision.HIGHEST
HIGH = lax.Precision.HIGH
GROUP = 64


def moduli(index, points):
    signed = jnp.where(index < points // 2, index, index - points).astype(jnp.float32) / points
    spline = 2.0 / 3.0 + jnp.cos(2.0 * math.pi / points * index.astype(jnp.float32)) / 3.0
    return (signed * signed, 1.0 / (spline * spline), index == points // 2)


def influence(first, second, third, points):
    sq_one, mod_one, edge_one = moduli(first, points)
    sq_two, mod_two, edge_two = moduli(second, points)
    sq_three, mod_three, edge_three = moduli(third, points)
    total = sq_one + sq_two + sq_three
    safe = jnp.where(total > 0.0, total, 1.0)
    value = (
        mod_one
        * mod_two
        * mod_three
        * jnp.exp(-(math.pi * math.pi / (SPLITTING * SPLITTING)) * total)
        / (math.pi * safe)
    )
    keep = (total > 0.0) & jnp.logical_not(edge_one | edge_two | edge_three)
    return jnp.where(keep, value, 0.0)


def spline_weights(frac):
    remain = 1.0 - frac
    square = frac * frac
    cubed = square * frac
    values = jnp.stack(
        [
            remain * remain * remain / 6.0,
            (3.0 * cubed - 6.0 * square + 4.0) / 6.0,
            (-3.0 * cubed + 3.0 * square + 3.0 * frac + 1.0) / 6.0,
            cubed / 6.0,
        ]
    )
    slopes = jnp.stack(
        [
            -0.5 * remain * remain,
            (3.0 * square - 4.0 * frac) / 2.0,
            (-3.0 * square + 2.0 * frac + 1.0) / 2.0,
            0.5 * square,
        ]
    )
    return (values, slopes)


def angle_tables(rows_in, cols_in, points):
    product = rows_in[:, None] * cols_in[None, :] % points
    angle = 2.0 * math.pi / points * product.astype(jnp.float32)
    return (jnp.cos(angle), jnp.sin(angle))


def line_tables(cells, values, slopes, extent):
    hits = (jnp.arange(extent, dtype=jnp.int32)[None, :, None] == cells[:, None, :]).astype(
        jnp.float32
    )
    return (jnp.sum(hits * values[:, None, :], axis=0), jnp.sum(hits * slopes[:, None, :], axis=0))


def spread_kernel(first_ref, count_ref, weights_ref, z_ref, y_ref, waves_ref, out_ref):
    half = pl.program_id(0)
    group = pl.program_id(1)

    @pl.when(group == 0)
    def _():
        out_ref[...] = jnp.zeros_like(out_ref)

    rows = out_ref.shape[1]
    weights = weights_ref[...]
    z_cell = z_ref[...]
    y_cell = y_ref[...]
    waves = waves_ref[...]
    high = waves.astype(jnp.bfloat16)
    low = (waves - high.astype(jnp.float32)).astype(jnp.bfloat16)
    first = first_ref[half, group]
    row_offset = lax.broadcasted_iota(jnp.int32, (rows, weights.shape[1]), 0) - y_cell

    def plane(step, carry):
        z = first + step
        offset = z - z_cell
        chosen = jnp.zeros((ORDER, weights.shape[1]), jnp.float32)
        for a in range(ORDER):
            chosen = jnp.where(offset == a, weights[a * ORDER : (a + 1) * ORDER], chosen)
        placed = jnp.zeros((rows, weights.shape[1]), jnp.float32)
        for b in range(ORDER):
            placed = jnp.where(row_offset == b, chosen[b : b + 1], placed)
        top = placed.astype(jnp.bfloat16)
        rest = (placed - top.astype(jnp.float32)).astype(jnp.bfloat16)
        total = jnp.dot(top, high, preferred_element_type=jnp.float32)
        total += jnp.dot(rest, high, preferred_element_type=jnp.float32)
        total += jnp.dot(top, low, preferred_element_type=jnp.float32)
        out_ref[z] += total
        return carry

    lax.fori_loop(0, count_ref[half, group], plane, 0)


def sort_by_plane(table, local_z):
    count = local_z.shape[0]
    order = jnp.arange(count, dtype=jnp.int32)
    before = (local_z[:, None] < local_z[None, :]) | (
        (local_z[:, None] == local_z[None, :]) & (order[:, None] < order[None, :])
    )
    rank = jnp.sum(before.astype(jnp.int32), axis=0)
    moves = (rank[:, None] == order[None, :]).astype(jnp.float32)
    return jnp.dot(table, moves, precision=HIGHEST)


def phases(cells, index, points):
    angle = (2.0 * math.pi / points) * (cells[..., None] * index % points).astype(jnp.float32)
    return (jnp.cos(angle), jnp.sin(angle))


def spread_lines(spread_weights, spread_base, z_first, y_first, z_extent, y_local, kx_index, points):
    count = spread_weights.shape[1]
    halves = lax.axis_size("gy")
    local = jnp.stack([spread_base[0] - z_first, spread_base[1] - y_first, spread_base[2]])
    table = jnp.concatenate([spread_weights, local.astype(jnp.float32)], axis=0)
    table = sort_by_plane(table, local[0])
    table = lax.all_gather(table, "gy")
    groups = count // GROUP
    width = ORDER * GROUP
    weights = table[:, : ORDER**3].reshape(halves, ORDER * ORDER, ORDER, groups, GROUP)
    weights = weights.transpose(0, 3, 1, 2, 4).reshape(halves, groups, ORDER * ORDER, width)
    cells = jnp.round(table[:, ORDER**3 :]).astype(jnp.int32).reshape(halves, 3, groups, GROUP)
    z_cell, y_cell, x_cell = cells[:, 0], cells[:, 1], cells[:, 2]
    first = jnp.min(z_cell, axis=-1)
    planes = jnp.max(z_cell, axis=-1) - first + ORDER
    z_wide = jnp.tile(z_cell, (1, 1, ORDER))[:, :, None, :]
    y_wide = jnp.tile(y_cell, (1, 1, ORDER))[:, :, None, :]
    cosine, sine = phases(x_cell, kx_index, points)
    step_cos, step_sin = phases(jnp.arange(ORDER, dtype=jnp.int32), kx_index, points)
    step_cos, step_sin = step_cos[:, None, :], step_sin[:, None, :]
    cosine, sine = cosine[:, :, None], sine[:, :, None]
    waves = jnp.concatenate(
        [cosine * step_cos - sine * step_sin, -(sine * step_cos + cosine * step_sin)], axis=-1
    ).reshape(halves, groups, width, -1)
    rows = -(-(y_local + ORDER - 1) // 8) * 8
    lanes = waves.shape[-1]
    per_group = lambda q, g, *_: (q, g, 0, 0)
    lines = pl.pallas_call(
        spread_kernel,
        grid_spec=pltpu.PrefetchScalarGridSpec(
            num_scalar_prefetch=2,
            grid=(halves, groups),
            in_specs=[
                pl.BlockSpec((None, None, ORDER * ORDER, width), per_group),
                pl.BlockSpec((None, None, 1, width), per_group),
                pl.BlockSpec((None, None, 1, width), per_group),
                pl.BlockSpec((None, None, width, lanes), per_group),
            ],
            out_specs=pl.BlockSpec((z_extent, None, rows, lanes), lambda q, g, *_: (0, q, 0, 0)),
        ),
        out_shape=jax.ShapeDtypeStruct((z_extent, halves, rows, lanes), jnp.float32),
        compiler_params=pltpu.CompilerParams(dimension_semantics=("arbitrary", "arbitrary")),
    )(first, planes, weights, z_wide, y_wide, waves)
    return lines, rows


def line_waves(cell, values, slopes, index, points):
    cosine, sine = phases(cell, index, points)
    step_cos, step_sin = phases(jnp.arange(ORDER, dtype=jnp.int32), index, points)
    found = []
    for table in (values, slopes):
        real = sum(table[c][..., None] * step_cos[c] for c in range(ORDER))
        imag = sum(table[c][..., None] * step_sin[c] for c in range(ORDER))
        found.append((cosine * real - sine * imag, cosine * imag + sine * real))
    return found


def slab_forces(lines, base, frac, z_first, y_index, x_index, points):
    z_extent, ky_local, _, kx_local = lines.shape
    shifts = jnp.arange(ORDER, dtype=jnp.int32)[:, None]
    w_z, d_z = spline_weights(frac[0])
    w_y, d_y = spline_weights(frac[1])
    w_x, d_x = spline_weights(frac[2])
    plane_w, plane_d = line_tables(base[0][None, :] - z_first + shifts, w_z, d_z, z_extent)
    (wy_re, wy_im), (dy_re, dy_im) = line_waves(base[1], w_y, d_y, y_index, points)
    (wx_re, wx_im), (dx_re, dx_im) = line_waves(base[2], w_x, d_x, x_index, points)
    join = lambda a, b: jnp.concatenate([a, b], axis=1)
    waves = jnp.stack([join(wx_re, -wx_im), join(wx_im, wx_re), join(dx_re, -dx_im), join(dx_im, dx_re)])
    count = base.shape[1]
    along = jnp.einsum(
        "mk,nk->mn",
        lines.reshape(z_extent * ky_local, 2 * kx_local),
        waves.reshape(4 * count, 2 * kx_local),
        precision=HIGH,
    ).reshape(z_extent, ky_local, 4, count)
    wy_re, wy_im, dy_re, dy_im = wy_re.T, wy_im.T, dy_re.T, dy_im.T
    plain = jnp.sum(along[:, :, 0] * wy_re - along[:, :, 1] * wy_im, axis=1)
    tilted = jnp.sum(along[:, :, 0] * dy_re - along[:, :, 1] * dy_im, axis=1)
    sloped = jnp.sum(along[:, :, 2] * wy_re - along[:, :, 3] * wy_im, axis=1)
    return jnp.stack(
        [
            jnp.sum(plain * plane_d, axis=0),
            jnp.sum(tilted * plane_w, axis=0),
            jnp.sum(sloped * plane_w, axis=0),
        ]
    )


def shards(spread_weights, spread_base, qm_base, qm_frac, qm_charge):
    points = GRID
    margin = ORDER - 1
    count_z = lax.axis_size("gz")
    count_y = lax.axis_size("gy")
    z_local = points // count_z
    y_local = points // count_y
    z_extent = z_local + margin
    kx_count = points // 2
    kx_local = kx_count // count_y
    ky_local = points // count_z
    z_first = lax.axis_index("gz") * z_local
    y_first = lax.axis_index("gy") * y_local
    ky_index = lax.axis_index("gz") * ky_local + jnp.arange(ky_local, dtype=jnp.int32)
    kx_index = lax.axis_index("gy") * kx_local + jnp.arange(kx_local, dtype=jnp.int32)
    positions = jnp.arange(points, dtype=jnp.int32)
    all_base = lax.all_gather(qm_base, ("gz", "gy"), axis=1, tiled=True)
    all_frac = lax.all_gather(qm_frac, ("gz", "gy"), axis=1, tiled=True)

    lines, rows = spread_lines(
        spread_weights, spread_base, z_first, y_first, z_extent, y_local, kx_index, points
    )
    row_cells = (
        jnp.arange(count_y, dtype=jnp.int32)[:, None] * y_local
        + jnp.arange(rows, dtype=jnp.int32)[None, :]
    ).reshape(-1) % points
    tables = jnp.concatenate(angle_tables(positions, row_cells, points), axis=0)
    lines = lines.reshape(z_extent, count_y * rows, 2 * kx_local)
    both = jnp.einsum("yr,zrk->zyk", tables, lines, precision=HIGH)
    with_cos, with_sin = both[:, :points], both[:, points:]
    packed = jnp.stack(
        [
            with_cos[:, :, :kx_local] + with_sin[:, :, kx_local:],
            with_cos[:, :, kx_local:] - with_sin[:, :, :kx_local],
        ],
        axis=1,
    )
    packed = packed.reshape(z_extent, 2, count_z, ky_local, kx_local).transpose(2, 0, 1, 3, 4)
    packed = packed.reshape(count_z, z_extent * 2 * ky_local * kx_local)
    moved = lax.all_to_all(packed, "gz", split_axis=0, concat_axis=0, tiled=True)

    z_cells = (
        jnp.arange(count_z, dtype=jnp.int32)[:, None] * z_local
        + jnp.arange(z_extent, dtype=jnp.int32)[None, :]
    ).reshape(-1) % points
    cells = ky_local * kx_local
    moved = moved.reshape(count_z * z_extent, 2 * cells)
    tables = jnp.concatenate(angle_tables(positions, z_cells, points), axis=0)
    both = jnp.dot(tables, moved, precision=HIGH).reshape(2, points, 2, ky_local, kx_local)
    green = influence(
        positions[:, None, None], ky_index[None, :, None], kx_index[None, None, :], points
    )
    kx_weight = jnp.where(kx_index == 0, 1.0, 2.0).astype(jnp.float32)
    green = green * (kx_weight * (1.0 / float(points * points * points)))
    spectrum = jnp.stack(
        [(both[0, :, 0] + both[1, :, 1]) * green, (both[0, :, 1] - both[1, :, 0]) * green], axis=1
    ).reshape(points, 2 * cells)
    back = jnp.concatenate(angle_tables(z_cells, positions, points), axis=0)
    both = jnp.dot(back, spectrum, precision=HIGH)
    both = both.reshape(2, count_z, z_extent, 2, ky_local, kx_local)
    lines = jnp.stack(
        [both[0, :, :, 0] - both[1, :, :, 1], both[0, :, :, 1] + both[1, :, :, 0]], axis=3
    )

    def one_slab(args):
        slab, base, frac, start = args
        return slab_forces(slab, base, frac, start, ky_index, kx_index, points)

    slab_base = all_base.reshape(3, count_z, -1).transpose(1, 0, 2)
    slab_frac = all_frac.reshape(3, count_z, -1).transpose(1, 0, 2)
    starts = jnp.arange(count_z, dtype=jnp.int32) * z_local
    partial = lax.map(one_slab, (lines, slab_base, slab_frac, starts))
    forces = lax.psum_scatter(
        partial.transpose(1, 0, 2).reshape(3, -1), ("gz", "gy"), scatter_dimension=1, tiled=True
    )
    return -qm_charge * forces


MESH = pl.DeviceIdType.MESH
RING = 4
PLANE = 4
LANES = 128
F32 = jnp.float32
BF16 = jnp.bfloat16
VMEM_LIMIT = 62 * 2**20


def split_table(table):
    high = table.astype(np.float32).astype(BF16)
    low = (table - high.astype(np.float64)).astype(np.float32).astype(BF16)
    return jnp.asarray(high), jnp.asarray(low)


def split(value):
    high = value.astype(BF16)
    return high, (value - high.astype(F32)).astype(BF16)


def dot3(a_high, a_low, b_high, b_low):
    total = jnp.dot(a_high, b_high, preferred_element_type=F32)
    total += jnp.dot(a_low, b_high, preferred_element_type=F32)
    return total + jnp.dot(a_high, b_low, preferred_element_type=F32)


def trig(units, points):
    rest = units - points * jnp.floor((units + 0.5) * (1.0 / points))
    quarter = points // 4
    turn = jnp.floor((rest + quarter / 2) * (1.0 / quarter))
    angle = (rest - quarter * turn) * (2.0 * math.pi / points)
    square = angle * angle
    sine = angle * (1.0 + square * (-1.0 / 6 + square * (1.0 / 120 + square * (-1.0 / 5040 + square / 362880))))
    cosine = 1.0 + square * (-0.5 + square * (1.0 / 24 + square * (-1.0 / 720 + square * (1.0 / 40320))))
    odd = (turn == 1.0) | (turn == 3.0)
    first = jnp.where(odd, sine, cosine)
    second = jnp.where(odd, cosine, sine)
    first = jnp.where((turn == 1.0) | (turn == 2.0), -first, first)
    second = jnp.where((turn == 2.0) | (turn == 3.0), -second, second)
    return first, second


def order_by(key, table):
    count = key.shape[0]
    order = jnp.arange(count, dtype=jnp.int32)
    before = (key[:, None] < key[None, :]) | ((key[:, None] == key[None, :]) & (order[:, None] < order[None, :]))
    rank = jnp.sum(before.astype(jnp.int32), axis=0)
    moves = (rank[:, None] == order[None, :]).astype(F32)
    return jnp.dot(table, moves, precision=HIGHEST)


PIECES = 3


def gather_kernel(own_ref, qm_ref, tab_ref, all_ref, zs, zr, xs, xr, ys, yr, fs, fr, gs, gr, qm_send, qm_recv):
    p = lax.axis_index("gz")
    y = lax.axis_index("gy")
    me = p * 2 + y
    total = RING * PLANE * 2
    ring, spot = p // PLANE, lax.rem(p, PLANE)
    x, core = spot // 2, lax.rem(spot, 2)
    barrier = pltpu.get_barrier_semaphore()
    for d in range(1, total):
        other = lax.rem(me + d, total)
        pl.semaphore_signal(barrier, inc=1, device_id=(other // 2, lax.rem(other, 2)), device_id_type=MESH)
    pl.semaphore_wait(barrier, total - 1)

    def place(z, xx, yy):
        return (z * 2 + xx) * 2 + yy

    def copy(src, dst, s, r, device):
        return pltpu.make_async_remote_copy(src_ref=src, dst_ref=dst, send_sem=s, recv_sem=r, device_id=device, device_id_type=MESH)

    above = (p + PLANE, y)
    below = (p - PLANE, y)
    aside = (ring * PLANE + (1 - x) * 2 + core, y)
    over = (p, 1 - y)
    cut = tab_ref.shape[1] // 16 * 8
    tab_ref[place(ring, x, y)] = own_ref[...]
    for d in range(1, total):
        other = lax.rem(me + d, total)
        copy(qm_ref, all_ref.at[me], qm_send, qm_recv, (other // 2, lax.rem(other, 2))).start()
    all_ref[me] = qm_ref[...]
    lower = (RING - 1 - ring) // 2
    near = ring + 1 - 2 * lax.rem(ring, 2)
    order = [ring, near, 1 + lower, (RING - 1) * lower]

    def go(copies):
        for c in copies:
            c.start()

    def pieces(src, dst, s, r, device):
        size = tab_ref.shape[1] // PIECES
        return [copy(src.at[pl.ds(k * size, size)], dst.at[pl.ds(k * size, size)], s, r, device) for k in range(PIECES)]

    def along_parts(z, i):
        src = own_ref if i == 0 else tab_ref.at[place(z, x, y)]
        dst = tab_ref.at[place(z, x, y)]
        return pieces(src, dst, zs.at[0, z], zr.at[z], above), pieces(src, dst, zs.at[1, z], zr.at[z], below)

    def flat_parts(z, i):
        src = own_ref if i == 0 else tab_ref.at[place(z, x, y)]
        dst = tab_ref.at[place(z, x, y)]
        both = zip(pieces(src, dst, xs.at[z], xr.at[z], aside), pieces(src, dst, ys.at[z], yr.at[z], over))
        return [c for pair in both for c in pair]

    def along(z, i):
        src = own_ref if i == 0 else tab_ref.at[place(z, x, y)]
        dst = tab_ref.at[place(z, x, y)]
        return copy(src, dst, zs.at[0, z], zr.at[z], above), copy(src, dst, zs.at[1, z], zr.at[z], below)

    def flat(z, i):
        src = own_ref if i == 0 else tab_ref.at[place(z, x, y)]
        dst = tab_ref.at[place(z, x, y)]
        return copy(src, dst, xs.at[z], xr.at[z], aside), copy(src, dst, ys.at[z], yr.at[z], over)

    def turn(z):
        first = tab_ref.at[place(z, 1 - x, y), pl.ds(0, cut)]
        second = tab_ref.at[place(z, x, 1 - y), pl.ds(cut, tab_ref.shape[1] - cut)]
        return copy(first, first, fs.at[z], fr.at[z], over), copy(second, second, gs.at[z], gr.at[z], aside)

    def corner(z):
        first = tab_ref.at[place(z, 1 - x, 1 - y), pl.ds(0, cut)]
        second = tab_ref.at[place(z, 1 - x, 1 - y), pl.ds(cut, tab_ref.shape[1] - cut)]
        return copy(first, first, fs.at[z], fr.at[z], over), copy(second, second, gs.at[z], gr.at[z], aside)

    def upward(z):
        return (z <= ring) & (ring < RING - 1)

    def downward(z):
        return (z >= ring) & (ring > 0)

    def relay(z):
        mine = tab_ref.at[place(z, 1 - x, y)]
        theirs = tab_ref.at[place(z, x, 1 - y)]
        copy(mine, mine, xs.at[z], xr.at[z], aside).wait_recv()
        copy(theirs, theirs, ys.at[z], yr.at[z], over).wait_recv()
        for c in turn(z):
            c.start()

    for i, z in enumerate(order):
        if i:
            along(z, i)[0].wait_recv()

        ups, downs = along_parts(z, i)

        @pl.when(upward(z))
        def _():
            go(ups)

        @pl.when(downward(z))
        def _():
            go(downs)

        go(flat_parts(z, i))
        if i:
            relay(order[i - 1])
    relay(order[-1])
    for i, z in enumerate(order):
        for c in corner(z):
            c.wait_recv()
    for i, z in enumerate(order):
        up, down = along(z, i)

        @pl.when(upward(z))
        def _():
            up.wait_send()

        @pl.when(downward(z))
        def _():
            down.wait_send()

        for c in flat(z, i) + turn(z):
            c.wait_send()
    rest = all_ref.at[pl.ds(0, total - 1)]
    copy(rest, rest, qm_send, qm_recv, over).wait()


def gather(own, qm):
    vmem = pl.BlockSpec(memory_space=pltpu.VMEM)
    ring = pltpu.SemaphoreType.DMA((RING,))
    single = pltpu.SemaphoreType.DMA
    return pl.pallas_call(
        gather_kernel,
        out_shape=(
            jax.ShapeDtypeStruct((RING * 4,) + own.shape, F32),
            jax.ShapeDtypeStruct((RING * PLANE * 2,) + qm.shape, F32),
        ),
        in_specs=[vmem] * 2,
        out_specs=(vmem, vmem),
        scratch_shapes=[pltpu.SemaphoreType.DMA((2, RING))] + [ring] * 9 + [single, single],
        compiler_params=pltpu.CompilerParams(collective_id=0, has_side_effects=True, vmem_limit_bytes=VMEM_LIMIT),
        name="gather_atoms",
    )(own, qm)


Z_STEP = 6
BLOCK = 256


def lines_kernel(points, kx_local, z_used, y_local, kx_ref, first_ref, count_ref, tab_ref, th_ref, tl_ref, out_ref, grid_ref):
    slab = pl.program_id(0)
    blocks = tab_ref.shape[2] // BLOCK
    modes = 2 * kx_local
    part = LANES // 2
    rows = ORDER * ORDER
    grid_ref[...] = jnp.zeros_like(grid_ref)
    lane = lax.broadcasted_iota(jnp.int32, (1, LANES), 1)
    mode = lax.broadcasted_iota(jnp.int32, (modes, LANES), 0)
    sine = mode >= kx_local
    kx = (kx_ref[0] + jnp.where(sine, mode - kx_local, mode)).astype(F32)
    shift = jnp.where(sine, points - points // 4, points).astype(F32)
    steps = [trig(kx * float(c), points) for c in range(ORDER)]
    wide = lax.broadcasted_iota(jnp.int32, (1, 2 * LANES), 1)
    y_shift = (wide // part).astype(F32)
    y_rows = lax.broadcasted_iota(jnp.int32, (2 * LANES, 2 * LANES), 0).astype(F32).astype(BF16)
    z_rows = lax.broadcasted_iota(jnp.int32, (8, 2 * LANES), 0)
    across = (((1,), (1,)), ((), ()))

    def some(i, outer):
        half = i // blocks
        at = lax.rem(i, blocks)
        sign = (1 - 2 * half).astype(F32)
        start = (ORDER - 1 + half * (y_local - 1)).astype(F32)
        base = (slab * 2 * blocks + i) * (BLOCK // part)
        most = count_ref[base]
        for g in range(1, BLOCK // part):
            most = jnp.maximum(most, count_ref[base + g])

        def step(it, carry):
            for t in range(BLOCK // LANES):
                tab = tab_ref[half, :, pl.ds(pl.multiple_of(at * BLOCK + t * LANES, LANES), LANES)]
                spots = tab[4 * rows : 4 * rows + 8]
                cosine, sinus = trig(kx * spots[2:3] + shift, points)
                waves = [cosine] + [cosine * steps[c][0] - sinus * steps[c][1] for c in range(1, ORDER)]
                rolled = [pltpu.roll(wave, part, 1) for wave in waves]
                turned = pltpu.roll(tab, part, 1)
                for h in range(2):
                    group = base + 2 * t + h

                    def pair(even, odd, even_turned, odd_turned):
                        if h == 0:
                            return jnp.where(lane < part, even, odd_turned)
                        return jnp.where(lane < part, even_turned, odd)

                    def cut(b):
                        return tab[b * rows : (b + 1) * rows], turned[b * rows : (b + 1) * rows]

                    def pick_pair(b):
                        even, even_turned = cut(b)
                        odd, odd_turned = cut(b + 1)
                        return pair(even, odd, even_turned, odd_turned)

                    weights = jnp.concatenate([pick_pair(0), pick_pair(2)], axis=1)
                    turned_spots = turned[4 * rows : 4 * rows + 8]
                    here = pair(spots, spots, turned_spots, turned_spots)
                    here = jnp.concatenate([here, here], axis=1)
                    z_first = first_ref[group] + it * Z_STEP
                    live = it < count_ref[group]
                    off = z_rows + jnp.where(live, z_first, 4 * points) - here[0:1].astype(jnp.int32)
                    z_first = jnp.minimum(z_first, z_used - 1)
                    picks = []
                    for c in range(ORDER):
                        pick = jnp.zeros((8, 2 * LANES), F32)
                        for a in range(ORDER):
                            pick = jnp.where(off == a, weights[a * ORDER + c : a * ORDER + c + 1], pick)
                        picks.append(pick)
                    own = [pair(wave, wave, back, back) for wave, back in zip(waves, rolled)]
                    own = [jnp.concatenate([wave, wave], axis=1) for wave in own]
                    pieces = []
                    for z in range(Z_STEP):
                        value = picks[0][z : z + 1] * own[0]
                        for c in range(1, ORDER):
                            value += picks[c][z : z + 1] * own[c]
                        pieces.append(value)
                    high, low = split(jnp.concatenate(pieces, axis=0))
                    y_cell = (start + sign * (here[1:2] + y_shift)).astype(BF16)
                    hits = jnp.where(y_rows == y_cell, jnp.ones((), BF16), jnp.zeros((), BF16))
                    total = lax.dot_general(high, hits, across, preferred_element_type=F32)
                    total += lax.dot_general(low, hits, across, preferred_element_type=F32)
                    grid_ref[half, pl.ds(pl.multiple_of(z_first * modes, 8), Z_STEP * modes), :] += total
            return carry

        lax.fori_loop(0, most, step, 0)
        return outer

    lax.fori_loop(0, 2 * blocks, some, 0)
    cuts = 3
    size = z_used * modes // cuts

    def chunk(i, carry):
        at = pl.multiple_of(i * size, 8)
        one, two = grid_ref[0, pl.ds(at, size), :], grid_ref[1, pl.ds(at, size), :]
        for k, value in enumerate((one + two, one - two)):
            high, low = split(value)
            found = dot3(high, low, th_ref[k], tl_ref[k])
            for t in range(2):
                out_ref[k, t, pl.ds(at, size), :] = found[:, t * LANES : (t + 1) * LANES]
        return carry

    lax.fori_loop(0, cuts, chunk, 0)


def spread(tab, kx_first, kx_local, z_local, y_local, points):
    tables, rows, count = tab.shape
    slabs = tables // 2
    part = LANES // 2
    z_used = z_local + ORDER - 1
    modes = 2 * kx_local
    z_cell = jnp.round(tab[:, 4 * ORDER * ORDER]).astype(jnp.int32).reshape(tables, count // part, part)
    first = jnp.min(z_cell, axis=-1)
    counts = (jnp.max(z_cell, axis=-1) - first + ORDER + Z_STEP - 1) // Z_STEP
    k = np.arange(points // 2)
    cell = 2 * (np.arange(2 * LANES) - (ORDER - 1)) + 1
    angle = np.pi / points * ((cell[:, None] * k) % (2 * points))
    table = np.zeros((2, 2 * LANES, 2 * LANES))
    table[0, :, : points // 2] = np.cos(angle)
    table[1, :, : points // 2] = np.sin(angle)
    th, tl = split_table(table)
    whole = lambda s, *_: (0, 0, 0)
    return pl.pallas_call(
        functools.partial(lines_kernel, points, kx_local, z_used, y_local),
        grid_spec=pltpu.PrefetchScalarGridSpec(
            num_scalar_prefetch=3,
            grid=(slabs,),
            in_specs=[
                pl.BlockSpec((None, 2, rows, count), lambda s, *_: (s, 0, 0, 0)),
                pl.BlockSpec(th.shape, whole),
                pl.BlockSpec(tl.shape, whole),
            ],
            out_specs=pl.BlockSpec((2, 2, None, z_used * modes, LANES), lambda s, *_: (0, 0, s, 0, 0)),
            scratch_shapes=[pltpu.VMEM((2, (z_used + Z_STEP - 1) * modes, 2 * LANES), F32)],
        ),
        out_shape=jax.ShapeDtypeStruct((2, 2, slabs, z_used * modes, LANES), F32),
        compiler_params=pltpu.CompilerParams(dimension_semantics=("arbitrary",), vmem_limit_bytes=VMEM_LIMIT),
        name="spread_lines",
    )(kx_first.reshape(1), first.reshape(-1), counts.reshape(-1), tab.reshape(slabs, 2, rows, count), th, tl)


def swap_kernel(lines_ref, out_ref, send_sem, recv_sem):
    p = lax.axis_index("gz")
    y = lax.axis_index("gy")
    core = lax.rem(p, 2)
    other = p + 1 - 2 * core
    barrier = pltpu.get_barrier_semaphore()
    pl.semaphore_signal(barrier, inc=1, device_id=(other, y), device_id_type=MESH)
    pl.semaphore_wait(barrier, 1)
    copies = []
    for t in range(out_ref.shape[0]):
        for i in range(out_ref.shape[1]):
            copies.append(pltpu.make_async_remote_copy(
                src_ref=lines_ref.at[1 - core, t, i], dst_ref=out_ref.at[t, i], send_sem=send_sem.at[t, i],
                recv_sem=recv_sem.at[t, i], device_id=(other, y), device_id_type=MESH))
            copies[-1].start()
    for copy in copies:
        copy.wait()


def swap(lines):
    types, tiles, slabs, deep, lanes = lines.shape
    space = pl.BlockSpec(memory_space=pl.ANY)
    return pl.pallas_call(
        swap_kernel,
        in_specs=[space],
        out_specs=space,
        out_shape=jax.ShapeDtypeStruct((tiles, slabs, deep, lanes), F32),
        scratch_shapes=[pltpu.SemaphoreType.DMA((tiles, slabs)), pltpu.SemaphoreType.DMA((tiles, slabs))],
        compiler_params=pltpu.CompilerParams(collective_id=1, has_side_effects=True, vmem_limit_bytes=VMEM_LIMIT),
        name="swap_modes",
    )(lines)


PACK = 4


def solve_kernel(points, kx_local, here_ref, x_ref, y_ref, fh_ref, fl_ref, bh_ref, bl_ref, az_ref, sz_ref, col_ref, sq_ref, qm_ref, out_ref, pot_ref, wave_h, wave_l, wx_ref, acc_ref, step_ref):
    modes = 2 * kx_local
    deep = y_ref.shape[1] // modes
    half = points // 2
    slabs = qm_ref.shape[0] // 2
    z_local = points // slabs
    atoms = 2 * qm_ref.shape[2]
    kx_first, core = here_ref[0], here_ref[1]
    y_shift = 2 * points - core * (points // 2)

    lane = lax.broadcasted_iota(jnp.int32, (1, LANES), 1)
    part = half - LANES
    wide = PACK * half // LANES
    for c in range(ORDER):
        ky_lane = lax.broadcasted_iota(jnp.int32, (half, LANES), 0).astype(F32)
        step_ref[c], step_ref[ORDER + c] = trig(ky_lane * float(c), points)

    def convolve(i, carry):
        def column(m, t):
            return jnp.concatenate(
                [x_ref[core, t, pl.ds(m, deep, stride=modes), :], y_ref[t, pl.ds(m, deep, stride=modes), :]], axis=0)

        heads = [column(PACK * i + j, 0) for j in range(PACK)]
        tails = [column(PACK * i + j, 1) for j in range(PACK)]
        tails = [jnp.where(lane < part, tails[j], pltpu.roll(tails[j + 1], part, 1)) for j in range(0, PACK, 2)]
        high, low = split(jnp.concatenate(heads + tails, axis=1))
        coef = dot3(fh_ref[core], fl_ref[core], high, low)
        total = jnp.concatenate([sz_ref[...]] * wide, axis=1) + sq_ref[pl.ds(i, 1), :]
        keep = total > 0.0
        value = jnp.concatenate([az_ref[...]] * wide, axis=1) * col_ref[pl.ds(i, 1), :] / jnp.where(keep, total, 1.0)
        green = jnp.where(keep, value, 0.0)
        high, low = split(coef * jnp.concatenate([green, green], axis=0))
        back = dot3(bh_ref[...], bl_ref[...], high, low)
        for j in range(PACK):
            pot_ref[PACK * i + j, :, :LANES] = back[:, j * LANES : (j + 1) * LANES]
            tail = back[:, (PACK + j // 2) * LANES : (PACK + j // 2 + 1) * LANES]
            pot_ref[PACK * i + j, :, LANES:] = pltpu.roll(tail, LANES - part, 1) if j % 2 else tail
        return carry

    lax.fori_loop(0, modes // PACK, convolve, 0)
    span = 4 * 8
    wave_h[half:] = jnp.zeros((2 * LANES - half, 2 * atoms), BF16)
    wave_l[half:] = jnp.zeros((2 * LANES - half, 2 * atoms), BF16)
    ky = lax.broadcasted_iota(jnp.int32, (half, atoms), 0).astype(F32)
    mode = lax.broadcasted_iota(jnp.int32, (modes, atoms), 0)
    sine = mode >= kx_local
    kx = (kx_first + jnp.where(sine, mode - kx_local, mode)).astype(F32)
    x_shift = jnp.where(sine, points - points // 4, points).astype(F32)

    def slab(p, carry):
        qm = jnp.concatenate([qm_ref[2 * p], qm_ref[2 * p + 1]], axis=1)
        values, slopes = spline_rows(qm)
        table = [qm[0:1], qm[1:2], qm[2:3]]
        for d in range(3, 6):
            for part in (values, slopes):
                table += [v[d : d + 1] for v in part]
        row = lambda i: table[i]
        cosine, sinus = trig(ky * (2.0 * row(1) + 1.0) + y_shift.astype(F32), 2 * points)
        for k, at in ((0, 11), (1, 15)):
            real = imag = None
            for c in range(ORDER):
                sc = jnp.concatenate([step_ref[c]] * (atoms // LANES), axis=1)
                ss = jnp.concatenate([step_ref[ORDER + c]] * (atoms // LANES), axis=1)
                real = row(at + c) * sc if real is None else real + row(at + c) * sc
                imag = row(at + c) * ss if imag is None else imag + row(at + c) * ss
            high, low = split(cosine * real - sinus * imag)
            wave_h[0:half, k * atoms : (k + 1) * atoms] = high
            wave_l[0:half, k * atoms : (k + 1) * atoms] = low
        plain_x = slope_x = jnp.zeros((modes, atoms), F32)
        for c in range(ORDER):
            wave, _ = trig(kx * (row(2) + float(c)) + x_shift, points)
            plain_x += row(19 + c) * wave
            slope_x += row(23 + c) * wave
        wx_ref[0] = plain_x
        wx_ref[1] = slope_x
        z_first = pl.multiple_of(p * z_local, 8)
        acc_ref[...] = jnp.zeros_like(acc_ref)
        for g in range(modes // 8):
            tiles = [pot_ref[g * 8 + i, pl.ds(z_first, span), :] for i in range(8)]
            high, low = split(jnp.concatenate(tiles, axis=0))
            along = dot3(high, low, wave_h[...], wave_l[...])
            for i in range(8):
                r = g * 8 + i
                value, slope = along[i * span : (i + 1) * span, :atoms], along[i * span : (i + 1) * span, atoms:]
                wx, dx = wx_ref[0, r : r + 1], wx_ref[1, r : r + 1]
                acc_ref[0] += value * wx
                acc_ref[1] += slope * wx
                acc_ref[2] += value * dx
        off = lax.broadcasted_iota(jnp.int32, (span, atoms), 0) + z_first - row(0).astype(jnp.int32)
        wz = dz = jnp.zeros((span, atoms), F32)
        for a in range(ORDER):
            wz = jnp.where(off == a, row(3 + a), wz)
            dz = jnp.where(off == a, row(7 + a), dz)
        total = lambda v: jnp.sum(v, axis=0, keepdims=True)
        found = jnp.concatenate(
            [total(acc_ref[0] * dz), total(acc_ref[1] * wz), total(acc_ref[2] * wz), jnp.zeros((5, atoms), F32)], axis=0)
        out_ref[2 * p] = found[:, : atoms // 2]
        out_ref[2 * p + 1] = found[:, atoms // 2 :]
        return carry

    lax.fori_loop(0, slabs, slab, 0)


def spline_rows(frac):
    remain = 1.0 - frac
    square = frac * frac
    cubed = square * frac
    values = [
        remain * remain * remain / 6.0,
        (3.0 * cubed - 6.0 * square + 4.0) / 6.0,
        (-3.0 * cubed + 3.0 * square + 3.0 * frac + 1.0) / 6.0,
        cubed / 6.0,
    ]
    slopes = [
        -0.5 * remain * remain,
        (3.0 * square - 4.0 * frac) / 2.0,
        (-3.0 * square + 2.0 * frac + 1.0) / 2.0,
        0.5 * square,
    ]
    return values, slopes


def solve(lines, other, here, qm_all, kx_index, points):
    tiles, slab_half, deep, lanes = other.shape
    kx_local = kx_index.shape[0]
    modes = 2 * kx_local
    half = points // 2
    slabs, atoms = qm_all.shape[0] // 2, 2 * qm_all.shape[2]
    z_local = points // slabs
    z_used = z_local + ORDER - 1
    k = np.arange(half)

    def waves(z):
        angle = 2.0 * np.pi / points * ((k[:, None] * z[None, :]) % points)
        return np.concatenate([np.cos(angle), np.sin(angle)], axis=0)

    core, pair, plane = np.meshgrid(np.arange(2), np.arange(slabs // 2), np.arange(z_used), indexing="ij")
    cells = (((pair * 2 + core) * z_local + plane) % points).reshape(2, -1)
    fh, fl = split_table(np.stack([waves(cells.reshape(-1)), waves(cells[::-1].reshape(-1))]))
    reach = points + 8
    bh, bl = split_table(waves(np.arange(reach) % points).T)

    def parts_of(index):
        square, spline, _ = moduli(index, points)
        decay = jnp.exp(-(math.pi * math.pi / (SPLITTING * SPLITTING)) * square)
        return square, spline * decay * jnp.where(index == 0, 1.0, 2.0)

    z_sq, z_fac = parts_of(jnp.asarray(k, jnp.int32))
    x_sq, x_fac = parts_of(jnp.concatenate([kx_index, kx_index]))

    def packed(table):
        table = table.reshape(modes // PACK, PACK, half)
        head = table[:, :, :lanes].reshape(modes // PACK, PACK * lanes)
        return jnp.concatenate([head, table[:, :, lanes:].reshape(modes // PACK, -1)], axis=1)

    col = packed(x_fac[:, None] * z_fac[None, :] * (1.0 / (math.pi * float(points) ** 3)))
    sq = packed(x_sq[:, None] + z_sq[None, :])
    az = jnp.broadcast_to(z_fac[:, None], (half, lanes))
    sz = jnp.broadcast_to(z_sq[:, None], (half, lanes))
    vmem = pl.BlockSpec(memory_space=pltpu.VMEM)
    return pl.pallas_call(
        functools.partial(solve_kernel, points, kx_local),
        in_specs=[pl.BlockSpec(memory_space=pltpu.SMEM)] + [vmem] * 11,
        out_specs=vmem,
        out_shape=jax.ShapeDtypeStruct((2 * slabs, 8, atoms // 2), F32),
        scratch_shapes=[
            pltpu.VMEM((modes, reach, 2 * lanes), F32),
            pltpu.VMEM((2 * lanes, 2 * atoms), BF16),
            pltpu.VMEM((2 * lanes, 2 * atoms), BF16),
            pltpu.VMEM((2, modes, atoms), F32),
            pltpu.VMEM((3, 32, atoms), F32),
            pltpu.VMEM((2 * ORDER, half, lanes), F32),
        ],
        compiler_params=pltpu.CompilerParams(vmem_limit_bytes=VMEM_LIMIT),
        name="solve_interpolate",
    )(here, lines.reshape(2, tiles, slab_half * deep, lanes), other.reshape(tiles, slab_half * deep, lanes), fh, fl, bh, bl, az, sz, col, sq, qm_all)


def reduce_kernel(count_z, count_y, part_ref, out_ref, land_ref, send_sem, recv_sem):
    p = lax.axis_index("gz")
    y = lax.axis_index("gy")
    me = p * count_y + y
    total = count_z * count_y
    width = out_ref.shape[1]
    barrier = pltpu.get_barrier_semaphore()
    for d in range(1, total):
        other = lax.rem(me + d, total)
        pl.semaphore_signal(barrier, inc=1, device_id=(other // count_y, lax.rem(other, count_y)), device_id_type=MESH)
    pl.semaphore_wait(barrier, total - 1)
    for d in range(1, total):
        other = lax.rem(me + d, total)
        pltpu.make_async_remote_copy(
            src_ref=part_ref.at[other], dst_ref=land_ref.at[me], send_sem=send_sem, recv_sem=recv_sem,
            device_id=(other // count_y, lax.rem(other, count_y)), device_id_type=MESH).start()
    land_ref[me] = part_ref[me]
    pltpu.make_async_remote_copy(
        src_ref=land_ref.at[pl.ds(0, total - 1)], dst_ref=land_ref.at[pl.ds(0, total - 1)], send_sem=send_sem, recv_sem=recv_sem,
        device_id=(p, 1 - y), device_id_type=MESH).wait()
    out_ref[...] = jnp.sum(land_ref[...], axis=0)


def reduce_forces(partial, count_z, count_y):
    total, rows, width = partial.shape
    vmem = pl.BlockSpec(memory_space=pltpu.VMEM)
    return pl.pallas_call(
        functools.partial(reduce_kernel, count_z, count_y),
        in_specs=[vmem],
        out_specs=vmem,
        out_shape=jax.ShapeDtypeStruct((rows, width), F32),
        scratch_shapes=[pltpu.VMEM((total, rows, width), F32), pltpu.SemaphoreType.DMA, pltpu.SemaphoreType.DMA],
        compiler_params=pltpu.CompilerParams(collective_id=2, has_side_effects=True, vmem_limit_bytes=VMEM_LIMIT),
        name="reduce_forces",
    )(partial)


def fast_shards(spread_weights, spread_base, qm_base, qm_frac, qm_charge):
    points = GRID
    count_z = lax.axis_size("gz")
    count_y = lax.axis_size("gy")
    z_local, y_local = points // count_z, points // count_y
    kx_local = points // (RING * PLANE * 2)
    p = lax.axis_index("gz")
    q = lax.axis_index("gy")
    count = spread_weights.shape[1]
    qm_count = qm_base.shape[1]

    z_cell = spread_base[0] - p * z_local
    y_cell = spread_base[1] - q * y_local
    cells = jnp.stack([z_cell, y_cell, spread_base[2]]).astype(F32)
    table = jnp.concatenate(
        [spread_weights.reshape(ORDER, ORDER, ORDER, count).transpose(1, 0, 2, 3).reshape(ORDER**3, count),
         cells, jnp.zeros((5, count), F32)], axis=0)
    own = order_by(z_cell, table)
    qm = jnp.concatenate([qm_base.astype(F32), qm_frac, jnp.zeros((2, qm_count), F32)], axis=0)
    tab, qm_all = gather(own, qm)

    kx_first = ((p // 2) * count_y + q) * kx_local
    lines = spread(tab, kx_first, kx_local, z_local, y_local, points)
    other = swap(lines)
    kx_index = kx_first + jnp.arange(kx_local, dtype=jnp.int32)
    partial = solve(lines, other, jnp.stack([kx_first, p % 2]), qm_all, kx_index, points)
    forces = reduce_forces(partial, count_z, count_y)
    return -qm_charge * forces[:3]


def quick(mesh):
    return mesh.shape["gz"] == RING * PLANE and mesh.shape["gy"] == 2


def solution(mesh):
    in_specs = (
        P(None, ("gz", "gy")),
        P(None, ("gz", "gy")),
        P(None, ("gz", "gy")),
        P(None, ("gz", "gy")),
        P(("gz", "gy")),
    )
    out_specs = P(None, ("gz", "gy"))
    body = fast_shards if quick(mesh) else shards
    return jax.shard_map(body, mesh=mesh, in_specs=in_specs, out_specs=out_specs, check_vma=False)
```

```python
import functools
import math

import jax
import jax.numpy as jnp
import numpy as np
from jax import lax
from jax.experimental import pallas as pl
from jax.experimental.pallas import tpu as pltpu
from jax.sharding import PartitionSpec as P

GRID = 384
ORDER = 4


SPLITTING = 0.8
HIGHEST = lax.Precision.HIGHEST
HIGH = lax.Precision.HIGH
GROUP = 64


def moduli(index, points):
    signed = jnp.where(index < points // 2, index, index - points).astype(jnp.float32) / points
    spline = 2.0 / 3.0 + jnp.cos(2.0 * math.pi / points * index.astype(jnp.float32)) / 3.0
    return (signed * signed, 1.0 / (spline * spline), index == points // 2)


def influence(first, second, third, points):
    sq_one, mod_one, edge_one = moduli(first, points)
    sq_two, mod_two, edge_two = moduli(second, points)
    sq_three, mod_three, edge_three = moduli(third, points)
    total = sq_one + sq_two + sq_three
    safe = jnp.where(total > 0.0, total, 1.0)
    value = (
        mod_one
        * mod_two
        * mod_three
        * jnp.exp(-(math.pi * math.pi / (SPLITTING * SPLITTING)) * total)
        / (math.pi * safe)
    )
    keep = (total > 0.0) & jnp.logical_not(edge_one | edge_two | edge_three)
    return jnp.where(keep, value, 0.0)


def spline_weights(frac):
    remain = 1.0 - frac
    square = frac * frac
    cubed = square * frac
    values = jnp.stack(
        [
            remain * remain * remain / 6.0,
            (3.0 * cubed - 6.0 * square + 4.0) / 6.0,
            (-3.0 * cubed + 3.0 * square + 3.0 * frac + 1.0) / 6.0,
            cubed / 6.0,
        ]
    )
    slopes = jnp.stack(
        [
            -0.5 * remain * remain,
            (3.0 * square - 4.0 * frac) / 2.0,
            (-3.0 * square + 2.0 * frac + 1.0) / 2.0,
            0.5 * square,
        ]
    )
    return (values, slopes)


def angle_tables(rows_in, cols_in, points):
    product = rows_in[:, None] * cols_in[None, :] % points
    angle = 2.0 * math.pi / points * product.astype(jnp.float32)
    return (jnp.cos(angle), jnp.sin(angle))


def line_tables(cells, values, slopes, extent):
    hits = (jnp.arange(extent, dtype=jnp.int32)[None, :, None] == cells[:, None, :]).astype(
        jnp.float32
    )
    return (jnp.sum(hits * values[:, None, :], axis=0), jnp.sum(hits * slopes[:, None, :], axis=0))


def spread_kernel(first_ref, count_ref, weights_ref, z_ref, y_ref, waves_ref, out_ref):
    half = pl.program_id(0)
    group = pl.program_id(1)

    @pl.when(group == 0)
    def _():
        out_ref[...] = jnp.zeros_like(out_ref)

    rows = out_ref.shape[1]
    weights = weights_ref[...]
    z_cell = z_ref[...]
    y_cell = y_ref[...]
    waves = waves_ref[...]
    high = waves.astype(jnp.bfloat16)
    low = (waves - high.astype(jnp.float32)).astype(jnp.bfloat16)
    first = first_ref[half, group]
    row_offset = lax.broadcasted_iota(jnp.int32, (rows, weights.shape[1]), 0) - y_cell

    def plane(step, carry):
        z = first + step
        offset = z - z_cell
        chosen = jnp.zeros((ORDER, weights.shape[1]), jnp.float32)
        for a in range(ORDER):
            chosen = jnp.where(offset == a, weights[a * ORDER : (a + 1) * ORDER], chosen)
        placed = jnp.zeros((rows, weights.shape[1]), jnp.float32)
        for b in range(ORDER):
            placed = jnp.where(row_offset == b, chosen[b : b + 1], placed)
        top = placed.astype(jnp.bfloat16)
        rest = (placed - top.astype(jnp.float32)).astype(jnp.bfloat16)
        total = jnp.dot(top, high, preferred_element_type=jnp.float32)
        total += jnp.dot(rest, high, preferred_element_type=jnp.float32)
        total += jnp.dot(top, low, preferred_element_type=jnp.float32)
        out_ref[z] += total
        return carry

    lax.fori_loop(0, count_ref[half, group], plane, 0)


def sort_by_plane(table, local_z):
    count = local_z.shape[0]
    order = jnp.arange(count, dtype=jnp.int32)
    before = (local_z[:, None] < local_z[None, :]) | (
        (local_z[:, None] == local_z[None, :]) & (order[:, None] < order[None, :])
    )
    rank = jnp.sum(before.astype(jnp.int32), axis=0)
    moves = (rank[:, None] == order[None, :]).astype(jnp.float32)
    return jnp.dot(table, moves, precision=HIGHEST)


def phases(cells, index, points):
    angle = (2.0 * math.pi / points) * (cells[..., None] * index % points).astype(jnp.float32)
    return (jnp.cos(angle), jnp.sin(angle))


def spread_lines(spread_weights, spread_base, z_first, y_first, z_extent, y_local, kx_index, points):
    count = spread_weights.shape[1]
    halves = lax.axis_size("gy")
    local = jnp.stack([spread_base[0] - z_first, spread_base[1] - y_first, spread_base[2]])
    table = jnp.concatenate([spread_weights, local.astype(jnp.float32)], axis=0)
    table = sort_by_plane(table, local[0])
    table = lax.all_gather(table, "gy")
    groups = count // GROUP
    width = ORDER * GROUP
    weights = table[:, : ORDER**3].reshape(halves, ORDER * ORDER, ORDER, groups, GROUP)
    weights = weights.transpose(0, 3, 1, 2, 4).reshape(halves, groups, ORDER * ORDER, width)
    cells = jnp.round(table[:, ORDER**3 :]).astype(jnp.int32).reshape(halves, 3, groups, GROUP)
    z_cell, y_cell, x_cell = cells[:, 0], cells[:, 1], cells[:, 2]
    first = jnp.min(z_cell, axis=-1)
    planes = jnp.max(z_cell, axis=-1) - first + ORDER
    z_wide = jnp.tile(z_cell, (1, 1, ORDER))[:, :, None, :]
    y_wide = jnp.tile(y_cell, (1, 1, ORDER))[:, :, None, :]
    cosine, sine = phases(x_cell, kx_index, points)
    step_cos, step_sin = phases(jnp.arange(ORDER, dtype=jnp.int32), kx_index, points)
    step_cos, step_sin = step_cos[:, None, :], step_sin[:, None, :]
    cosine, sine = cosine[:, :, None], sine[:, :, None]
    waves = jnp.concatenate(
        [cosine * step_cos - sine * step_sin, -(sine * step_cos + cosine * step_sin)], axis=-1
    ).reshape(halves, groups, width, -1)
    rows = -(-(y_local + ORDER - 1) // 8) * 8
    lanes = waves.shape[-1]
    per_group = lambda q, g, *_: (q, g, 0, 0)
    lines = pl.pallas_call(
        spread_kernel,
        grid_spec=pltpu.PrefetchScalarGridSpec(
            num_scalar_prefetch=2,
            grid=(halves, groups),
            in_specs=[
                pl.BlockSpec((None, None, ORDER * ORDER, width), per_group),
                pl.BlockSpec((None, None, 1, width), per_group),
                pl.BlockSpec((None, None, 1, width), per_group),
                pl.BlockSpec((None, None, width, lanes), per_group),
            ],
            out_specs=pl.BlockSpec((z_extent, None, rows, lanes), lambda q, g, *_: (0, q, 0, 0)),
        ),
        out_shape=jax.ShapeDtypeStruct((z_extent, halves, rows, lanes), jnp.float32),
        compiler_params=pltpu.CompilerParams(dimension_semantics=("arbitrary", "arbitrary")),
    )(first, planes, weights, z_wide, y_wide, waves)
    return lines, rows


def line_waves(cell, values, slopes, index, points):
    cosine, sine = phases(cell, index, points)
    step_cos, step_sin = phases(jnp.arange(ORDER, dtype=jnp.int32), index, points)
    found = []
    for table in (values, slopes):
        real = sum(table[c][..., None] * step_cos[c] for c in range(ORDER))
        imag = sum(table[c][..., None] * step_sin[c] for c in range(ORDER))
        found.append((cosine * real - sine * imag, cosine * imag + sine * real))
    return found


def slab_forces(lines, base, frac, z_first, y_index, x_index, points):
    z_extent, ky_local, _, kx_local = lines.shape
    shifts = jnp.arange(ORDER, dtype=jnp.int32)[:, None]
    w_z, d_z = spline_weights(frac[0])
    w_y, d_y = spline_weights(frac[1])
    w_x, d_x = spline_weights(frac[2])
    plane_w, plane_d = line_tables(base[0][None, :] - z_first + shifts, w_z, d_z, z_extent)
    (wy_re, wy_im), (dy_re, dy_im) = line_waves(base[1], w_y, d_y, y_index, points)
    (wx_re, wx_im), (dx_re, dx_im) = line_waves(base[2], w_x, d_x, x_index, points)
    join = lambda a, b: jnp.concatenate([a, b], axis=1)
    waves = jnp.stack([join(wx_re, -wx_im), join(wx_im, wx_re), join(dx_re, -dx_im), join(dx_im, dx_re)])
    count = base.shape[1]
    along = jnp.einsum(
        "mk,nk->mn",
        lines.reshape(z_extent * ky_local, 2 * kx_local),
        waves.reshape(4 * count, 2 * kx_local),
        precision=HIGH,
    ).reshape(z_extent, ky_local, 4, count)
    wy_re, wy_im, dy_re, dy_im = wy_re.T, wy_im.T, dy_re.T, dy_im.T
    plain = jnp.sum(along[:, :, 0] * wy_re - along[:, :, 1] * wy_im, axis=1)
    tilted = jnp.sum(along[:, :, 0] * dy_re - along[:, :, 1] * dy_im, axis=1)
    sloped = jnp.sum(along[:, :, 2] * wy_re - along[:, :, 3] * wy_im, axis=1)
    return jnp.stack(
        [
            jnp.sum(plain * plane_d, axis=0),
            jnp.sum(tilted * plane_w, axis=0),
            jnp.sum(sloped * plane_w, axis=0),
        ]
    )


def shards(spread_weights, spread_base, qm_base, qm_frac, qm_charge):
    points = GRID
    margin = ORDER - 1
    count_z = lax.axis_size("gz")
    count_y = lax.axis_size("gy")
    z_local = points // count_z
    y_local = points // count_y
    z_extent = z_local + margin
    kx_count = points // 2
    kx_local = kx_count // count_y
    ky_local = points // count_z
    z_first = lax.axis_index("gz") * z_local
    y_first = lax.axis_index("gy") * y_local
    ky_index = lax.axis_index("gz") * ky_local + jnp.arange(ky_local, dtype=jnp.int32)
    kx_index = lax.axis_index("gy") * kx_local + jnp.arange(kx_local, dtype=jnp.int32)
    positions = jnp.arange(points, dtype=jnp.int32)
    all_base = lax.all_gather(qm_base, ("gz", "gy"), axis=1, tiled=True)
    all_frac = lax.all_gather(qm_frac, ("gz", "gy"), axis=1, tiled=True)

    lines, rows = spread_lines(
        spread_weights, spread_base, z_first, y_first, z_extent, y_local, kx_index, points
    )
    row_cells = (
        jnp.arange(count_y, dtype=jnp.int32)[:, None] * y_local
        + jnp.arange(rows, dtype=jnp.int32)[None, :]
    ).reshape(-1) % points
    tables = jnp.concatenate(angle_tables(positions, row_cells, points), axis=0)
    lines = lines.reshape(z_extent, count_y * rows, 2 * kx_local)
    both = jnp.einsum("yr,zrk->zyk", tables, lines, precision=HIGH)
    with_cos, with_sin = both[:, :points], both[:, points:]
    packed = jnp.stack(
        [
            with_cos[:, :, :kx_local] + with_sin[:, :, kx_local:],
            with_cos[:, :, kx_local:] - with_sin[:, :, :kx_local],
        ],
        axis=1,
    )
    packed = packed.reshape(z_extent, 2, count_z, ky_local, kx_local).transpose(2, 0, 1, 3, 4)
    packed = packed.reshape(count_z, z_extent * 2 * ky_local * kx_local)
    moved = lax.all_to_all(packed, "gz", split_axis=0, concat_axis=0, tiled=True)

    z_cells = (
        jnp.arange(count_z, dtype=jnp.int32)[:, None] * z_local
        + jnp.arange(z_extent, dtype=jnp.int32)[None, :]
    ).reshape(-1) % points
    cells = ky_local * kx_local
    moved = moved.reshape(count_z * z_extent, 2 * cells)
    tables = jnp.concatenate(angle_tables(positions, z_cells, points), axis=0)
    both = jnp.dot(tables, moved, precision=HIGH).reshape(2, points, 2, ky_local, kx_local)
    green = influence(
        positions[:, None, None], ky_index[None, :, None], kx_index[None, None, :], points
    )
    kx_weight = jnp.where(kx_index == 0, 1.0, 2.0).astype(jnp.float32)
    green = green * (kx_weight * (1.0 / float(points * points * points)))
    spectrum = jnp.stack(
        [(both[0, :, 0] + both[1, :, 1]) * green, (both[0, :, 1] - both[1, :, 0]) * green], axis=1
    ).reshape(points, 2 * cells)
    back = jnp.concatenate(angle_tables(z_cells, positions, points), axis=0)
    both = jnp.dot(back, spectrum, precision=HIGH)
    both = both.reshape(2, count_z, z_extent, 2, ky_local, kx_local)
    lines = jnp.stack(
        [both[0, :, :, 0] - both[1, :, :, 1], both[0, :, :, 1] + both[1, :, :, 0]], axis=3
    )

    def one_slab(args):
        slab, base, frac, start = args
        return slab_forces(slab, base, frac, start, ky_index, kx_index, points)

    slab_base = all_base.reshape(3, count_z, -1).transpose(1, 0, 2)
    slab_frac = all_frac.reshape(3, count_z, -1).transpose(1, 0, 2)
    starts = jnp.arange(count_z, dtype=jnp.int32) * z_local
    partial = lax.map(one_slab, (lines, slab_base, slab_frac, starts))
    forces = lax.psum_scatter(
        partial.transpose(1, 0, 2).reshape(3, -1), ("gz", "gy"), scatter_dimension=1, tiled=True
    )
    return -qm_charge * forces


MESH = pl.DeviceIdType.MESH
RING = 4
PLANE = 4
LANES = 128
F32 = jnp.float32
BF16 = jnp.bfloat16
VMEM_LIMIT = 62 * 2**20


def split_table(table):
    high = table.astype(np.float32).astype(BF16)
    low = (table - high.astype(np.float64)).astype(np.float32).astype(BF16)
    return jnp.asarray(high), jnp.asarray(low)


def split(value):
    high = value.astype(BF16)
    return high, (value - high.astype(F32)).astype(BF16)


def dot3(a_high, a_low, b_high, b_low):
    total = jnp.dot(a_high, b_high, preferred_element_type=F32)
    total += jnp.dot(a_low, b_high, preferred_element_type=F32)
    return total + jnp.dot(a_high, b_low, preferred_element_type=F32)


def trig(units, points):
    rest = units - points * jnp.floor((units + 0.5) * (1.0 / points))
    quarter = points // 4
    turn = jnp.floor((rest + quarter / 2) * (1.0 / quarter))
    angle = (rest - quarter * turn) * (2.0 * math.pi / points)
    square = angle * angle
    sine = angle * (1.0 + square * (-1.0 / 6 + square * (1.0 / 120 + square * (-1.0 / 5040 + square / 362880))))
    cosine = 1.0 + square * (-0.5 + square * (1.0 / 24 + square * (-1.0 / 720 + square * (1.0 / 40320))))
    odd = (turn == 1.0) | (turn == 3.0)
    first = jnp.where(odd, sine, cosine)
    second = jnp.where(odd, cosine, sine)
    first = jnp.where((turn == 1.0) | (turn == 2.0), -first, first)
    second = jnp.where((turn == 2.0) | (turn == 3.0), -second, second)
    return first, second


def order_by(key, table):
    count = key.shape[0]
    order = jnp.arange(count, dtype=jnp.int32)
    before = (key[:, None] < key[None, :]) | ((key[:, None] == key[None, :]) & (order[:, None] < order[None, :]))
    rank = jnp.sum(before.astype(jnp.int32), axis=0)
    moves = (rank[:, None] == order[None, :]).astype(F32)
    return jnp.dot(table, moves, precision=HIGHEST)


PIECES = 3


def gather_kernel(own_ref, qm_ref, tab_ref, all_ref, zs, zr, xs, xr, ys, yr, fs, fr, gs, gr, qm_send, qm_recv):
    p = lax.axis_index("gz")
    y = lax.axis_index("gy")
    me = p * 2 + y
    total = RING * PLANE * 2
    ring, spot = p // PLANE, lax.rem(p, PLANE)
    x, core = spot // 2, lax.rem(spot, 2)
    barrier = pltpu.get_barrier_semaphore()
    for d in range(1, total):
        other = lax.rem(me + d, total)
        pl.semaphore_signal(barrier, inc=1, device_id=(other // 2, lax.rem(other, 2)), device_id_type=MESH)
    pl.semaphore_wait(barrier, total - 1)

    def place(z, xx, yy):
        return (z * 2 + xx) * 2 + yy

    def copy(src, dst, s, r, device):
        return pltpu.make_async_remote_copy(src_ref=src, dst_ref=dst, send_sem=s, recv_sem=r, device_id=device, device_id_type=MESH)

    above = (p + PLANE, y)
    below = (p - PLANE, y)
    aside = (ring * PLANE + (1 - x) * 2 + core, y)
    over = (p, 1 - y)
    cut = tab_ref.shape[1] // 16 * 8
    tab_ref[place(ring, x, y)] = own_ref[...]
    for d in range(1, total):
        other = lax.rem(me + d, total)
        copy(qm_ref, all_ref.at[me], qm_send, qm_recv, (other // 2, lax.rem(other, 2))).start()
    all_ref[me] = qm_ref[...]
    lower = (RING - 1 - ring) // 2
    near = ring + 1 - 2 * lax.rem(ring, 2)
    order = [ring, near, 1 + lower, (RING - 1) * lower]

    def go(copies):
        for c in copies:
            c.start()

    def pieces(src, dst, s, r, device):
        size = tab_ref.shape[1] // PIECES
        return [copy(src.at[pl.ds(k * size, size)], dst.at[pl.ds(k * size, size)], s, r, device) for k in range(PIECES)]

    def along_parts(z, i):
        src = own_ref if i == 0 else tab_ref.at[place(z, x, y)]
        dst = tab_ref.at[place(z, x, y)]
        return pieces(src, dst, zs.at[0, z], zr.at[z], above), pieces(src, dst, zs.at[1, z], zr.at[z], below)

    def flat_parts(z, i):
        src = own_ref if i == 0 else tab_ref.at[place(z, x, y)]
        dst = tab_ref.at[place(z, x, y)]
        both = zip(pieces(src, dst, xs.at[z], xr.at[z], aside), pieces(src, dst, ys.at[z], yr.at[z], over))
        return [c for pair in both for c in pair]

    def along(z, i):
        src = own_ref if i == 0 else tab_ref.at[place(z, x, y)]
        dst = tab_ref.at[place(z, x, y)]
        return copy(src, dst, zs.at[0, z], zr.at[z], above), copy(src, dst, zs.at[1, z], zr.at[z], below)

    def flat(z, i):
        src = own_ref if i == 0 else tab_ref.at[place(z, x, y)]
        dst = tab_ref.at[place(z, x, y)]
        return copy(src, dst, xs.at[z], xr.at[z], aside), copy(src, dst, ys.at[z], yr.at[z], over)

    def turn(z):
        first = tab_ref.at[place(z, 1 - x, y), pl.ds(0, cut)]
        second = tab_ref.at[place(z, x, 1 - y), pl.ds(cut, tab_ref.shape[1] - cut)]
        return copy(first, first, fs.at[z], fr.at[z], over), copy(second, second, gs.at[z], gr.at[z], aside)

    def corner(z):
        first = tab_ref.at[place(z, 1 - x, 1 - y), pl.ds(0, cut)]
        second = tab_ref.at[place(z, 1 - x, 1 - y), pl.ds(cut, tab_ref.shape[1] - cut)]
        return copy(first, first, fs.at[z], fr.at[z], over), copy(second, second, gs.at[z], gr.at[z], aside)

    def upward(z):
        return (z <= ring) & (ring < RING - 1)

    def downward(z):
        return (z >= ring) & (ring > 0)

    def relay(z):
        mine = tab_ref.at[place(z, 1 - x, y)]
        theirs = tab_ref.at[place(z, x, 1 - y)]
        copy(mine, mine, xs.at[z], xr.at[z], aside).wait_recv()
        copy(theirs, theirs, ys.at[z], yr.at[z], over).wait_recv()
        for c in turn(z):
            c.start()

    for i, z in enumerate(order):
        if i:
            along(z, i)[0].wait_recv()

        ups, downs = along_parts(z, i)

        @pl.when(upward(z))
        def _():
            go(ups)

        @pl.when(downward(z))
        def _():
            go(downs)

        go(flat_parts(z, i))
        if i:
            relay(order[i - 1])
    relay(order[-1])
    for i, z in enumerate(order):
        for c in corner(z):
            c.wait_recv()
    for i, z in enumerate(order):
        up, down = along(z, i)

        @pl.when(upward(z))
        def _():
            up.wait_send()

        @pl.when(downward(z))
        def _():
            down.wait_send()

        for c in flat(z, i) + turn(z):
            c.wait_send()
    rest = all_ref.at[pl.ds(0, total - 1)]
    copy(rest, rest, qm_send, qm_recv, over).wait()


def gather(own, qm):
    vmem = pl.BlockSpec(memory_space=pltpu.VMEM)
    ring = pltpu.SemaphoreType.DMA((RING,))
    single = pltpu.SemaphoreType.DMA
    return pl.pallas_call(
        gather_kernel,
        out_shape=(
            jax.ShapeDtypeStruct((RING * 4,) + own.shape, F32),
            jax.ShapeDtypeStruct((RING * PLANE * 2,) + qm.shape, F32),
        ),
        in_specs=[vmem] * 2,
        out_specs=(vmem, vmem),
        scratch_shapes=[pltpu.SemaphoreType.DMA((2, RING))] + [ring] * 9 + [single, single],
        compiler_params=pltpu.CompilerParams(collective_id=0, has_side_effects=True, vmem_limit_bytes=VMEM_LIMIT),
        name="gather_atoms",
    )(own, qm)


Z_STEP = 6
BLOCK = 512


def lines_kernel(points, kx_local, z_used, y_local, kx_ref, first_ref, count_ref, tab_ref, th_ref, tl_ref, out_ref, grid_ref):
    slab = pl.program_id(0)
    blocks = tab_ref.shape[2] // BLOCK
    modes = 2 * kx_local
    part = LANES // 2
    rows = ORDER * ORDER
    grid_ref[...] = jnp.zeros_like(grid_ref)
    lane = lax.broadcasted_iota(jnp.int32, (1, LANES), 1)
    mode = lax.broadcasted_iota(jnp.int32, (modes, LANES), 0)
    sine = mode >= kx_local
    kx = (kx_ref[0] + jnp.where(sine, mode - kx_local, mode)).astype(F32)
    shift = jnp.where(sine, points - points // 4, points).astype(F32)
    steps = [trig(kx * float(c), points) for c in range(ORDER)]
    wide = lax.broadcasted_iota(jnp.int32, (1, 2 * LANES), 1)
    y_shift = (wide // part).astype(F32)
    y_rows = lax.broadcasted_iota(jnp.int32, (2 * LANES, 2 * LANES), 0).astype(F32).astype(BF16)
    z_rows = lax.broadcasted_iota(jnp.int32, (8, 2 * LANES), 0)
    across = (((1,), (1,)), ((), ()))

    def some(i, outer):
        half = i // blocks
        at = lax.rem(i, blocks)
        sign = (1 - 2 * half).astype(F32)
        start = (ORDER - 1 + half * (y_local - 1)).astype(F32)
        base = (slab * 2 * blocks + i) * (BLOCK // part)
        most = count_ref[base]
        for g in range(1, BLOCK // part):
            most = jnp.maximum(most, count_ref[base + g])

        def step(it, carry):
            for t in range(BLOCK // LANES):
                tab = tab_ref[half, :, pl.ds(pl.multiple_of(at * BLOCK + t * LANES, LANES), LANES)]
                spots = tab[4 * rows : 4 * rows + 8]
                cosine, sinus = trig(kx * spots[2:3] + shift, points)
                waves = [cosine] + [cosine * steps[c][0] - sinus * steps[c][1] for c in range(1, ORDER)]
                rolled = [pltpu.roll(wave, part, 1) for wave in waves]
                turned = pltpu.roll(tab, part, 1)
                for h in range(2):
                    group = base + 2 * t + h

                    def pair(even, odd, even_turned, odd_turned):
                        if h == 0:
                            return jnp.where(lane < part, even, odd_turned)
                        return jnp.where(lane < part, even_turned, odd)

                    def cut(b):
                        return tab[b * rows : (b + 1) * rows], turned[b * rows : (b + 1) * rows]

                    def pick_pair(b):
                        even, even_turned = cut(b)
                        odd, odd_turned = cut(b + 1)
                        return pair(even, odd, even_turned, odd_turned)

                    weights = jnp.concatenate([pick_pair(0), pick_pair(2)], axis=1)
                    turned_spots = turned[4 * rows : 4 * rows + 8]
                    here = pair(spots, spots, turned_spots, turned_spots)
                    here = jnp.concatenate([here, here], axis=1)
                    z_first = first_ref[group] + it * Z_STEP
                    live = it < count_ref[group]
                    off = z_rows + jnp.where(live, z_first, 4 * points) - here[0:1].astype(jnp.int32)
                    z_first = jnp.minimum(z_first, z_used - 1)
                    picks = []
                    for c in range(ORDER):
                        pick = jnp.zeros((8, 2 * LANES), F32)
                        for a in range(ORDER):
                            pick = jnp.where(off == a, weights[a * ORDER + c : a * ORDER + c + 1], pick)
                        picks.append(pick)
                    own = [pair(wave, wave, back, back) for wave, back in zip(waves, rolled)]
                    own = [jnp.concatenate([wave, wave], axis=1) for wave in own]
                    pieces = []
                    for z in range(Z_STEP):
                        value = picks[0][z : z + 1] * own[0]
                        for c in range(1, ORDER):
                            value += picks[c][z : z + 1] * own[c]
                        pieces.append(value)
                    high, low = split(jnp.concatenate(pieces, axis=0))
                    y_cell = (start + sign * (here[1:2] + y_shift)).astype(BF16)
                    hits = jnp.where(y_rows == y_cell, jnp.ones((), BF16), jnp.zeros((), BF16))
                    total = lax.dot_general(high, hits, across, preferred_element_type=F32)
                    total += lax.dot_general(low, hits, across, preferred_element_type=F32)
                    grid_ref[half, pl.ds(pl.multiple_of(z_first * modes, 8), Z_STEP * modes), :] += total
            return carry

        lax.fori_loop(0, most, step, 0)
        return outer

    lax.fori_loop(0, 2 * blocks, some, 0)
    cuts = 3
    size = z_used * modes // cuts

    def chunk(i, carry):
        at = pl.multiple_of(i * size, 8)
        one, two = grid_ref[0, pl.ds(at, size), :], grid_ref[1, pl.ds(at, size), :]
        for k, value in enumerate((one + two, one - two)):
            high, low = split(value)
            found = dot3(high, low, th_ref[k], tl_ref[k])
            for t in range(2):
                out_ref[k, t, pl.ds(at, size), :] = found[:, t * LANES : (t + 1) * LANES]
        return carry

    lax.fori_loop(0, cuts, chunk, 0)


def spread(tab, kx_first, kx_local, z_local, y_local, points):
    tables, rows, count = tab.shape
    slabs = tables // 2
    part = LANES // 2
    z_used = z_local + ORDER - 1
    modes = 2 * kx_local
    z_cell = jnp.round(tab[:, 4 * ORDER * ORDER]).astype(jnp.int32).reshape(tables, count // part, part)
    first = jnp.min(z_cell, axis=-1)
    counts = (jnp.max(z_cell, axis=-1) - first + ORDER + Z_STEP - 1) // Z_STEP
    k = np.arange(points // 2)
    cell = 2 * (np.arange(2 * LANES) - (ORDER - 1)) + 1
    angle = np.pi / points * ((cell[:, None] * k) % (2 * points))
    table = np.zeros((2, 2 * LANES, 2 * LANES))
    table[0, :, : points // 2] = np.cos(angle)
    table[1, :, : points // 2] = np.sin(angle)
    th, tl = split_table(table)
    whole = lambda s, *_: (0, 0, 0)
    return pl.pallas_call(
        functools.partial(lines_kernel, points, kx_local, z_used, y_local),
        grid_spec=pltpu.PrefetchScalarGridSpec(
            num_scalar_prefetch=3,
            grid=(slabs,),
            in_specs=[
                pl.BlockSpec((None, 2, rows, count), lambda s, *_: (s, 0, 0, 0)),
                pl.BlockSpec(th.shape, whole),
                pl.BlockSpec(tl.shape, whole),
            ],
            out_specs=pl.BlockSpec((2, 2, None, z_used * modes, LANES), lambda s, *_: (0, 0, s, 0, 0)),
            scratch_shapes=[pltpu.VMEM((2, (z_used + Z_STEP - 1) * modes, 2 * LANES), F32)],
        ),
        out_shape=jax.ShapeDtypeStruct((2, 2, slabs, z_used * modes, LANES), F32),
        compiler_params=pltpu.CompilerParams(dimension_semantics=("arbitrary",), vmem_limit_bytes=VMEM_LIMIT),
        name="spread_lines",
    )(kx_first.reshape(1), first.reshape(-1), counts.reshape(-1), tab.reshape(slabs, 2, rows, count), th, tl)


def swap_kernel(lines_ref, out_ref, send_sem, recv_sem):
    p = lax.axis_index("gz")
    y = lax.axis_index("gy")
    core = lax.rem(p, 2)
    other = p + 1 - 2 * core
    barrier = pltpu.get_barrier_semaphore()
    pl.semaphore_signal(barrier, inc=1, device_id=(other, y), device_id_type=MESH)
    pl.semaphore_wait(barrier, 1)
    copies = []
    for t in range(out_ref.shape[0]):
        for i in range(out_ref.shape[1]):
            copies.append(pltpu.make_async_remote_copy(
                src_ref=lines_ref.at[1 - core, t, i], dst_ref=out_ref.at[t, i], send_sem=send_sem.at[t, i],
                recv_sem=recv_sem.at[t, i], device_id=(other, y), device_id_type=MESH))
            copies[-1].start()
    for copy in copies:
        copy.wait()


def swap(lines):
    types, tiles, slabs, deep, lanes = lines.shape
    space = pl.BlockSpec(memory_space=pl.ANY)
    return pl.pallas_call(
        swap_kernel,
        in_specs=[space],
        out_specs=space,
        out_shape=jax.ShapeDtypeStruct((tiles, slabs, deep, lanes), F32),
        scratch_shapes=[pltpu.SemaphoreType.DMA((tiles, slabs)), pltpu.SemaphoreType.DMA((tiles, slabs))],
        compiler_params=pltpu.CompilerParams(collective_id=1, has_side_effects=True, vmem_limit_bytes=VMEM_LIMIT),
        name="swap_modes",
    )(lines)


PACK = 8


def solve_kernel(points, kx_local, here_ref, x_ref, y_ref, fh_ref, fl_ref, bh_ref, bl_ref, az_ref, sz_ref, col_ref, sq_ref, qm_ref, out_ref, pot_ref, wave_h, wave_l, wx_ref, acc_ref, step_ref):
    modes = 2 * kx_local
    deep = y_ref.shape[1] // modes
    half = points // 2
    slabs = qm_ref.shape[0] // 2
    z_local = points // slabs
    atoms = 2 * qm_ref.shape[2]
    kx_first, core = here_ref[0], here_ref[1]
    y_shift = 2 * points - core * (points // 2)

    lane = lax.broadcasted_iota(jnp.int32, (1, LANES), 1)
    part = half - LANES
    wide = PACK * half // LANES
    for c in range(ORDER):
        ky_lane = lax.broadcasted_iota(jnp.int32, (half, LANES), 0).astype(F32)
        step_ref[c], step_ref[ORDER + c] = trig(ky_lane * float(c), points)

    def convolve(i, carry):
        def column(m, t):
            return jnp.concatenate(
                [x_ref[core, t, pl.ds(m, deep, stride=modes), :], y_ref[t, pl.ds(m, deep, stride=modes), :]], axis=0)

        heads = [column(PACK * i + j, 0) for j in range(PACK)]
        tails = [column(PACK * i + j, 1) for j in range(PACK)]
        tails = [jnp.where(lane < part, tails[j], pltpu.roll(tails[j + 1], part, 1)) for j in range(0, PACK, 2)]
        high, low = split(jnp.concatenate(heads + tails, axis=1))
        coef = dot3(fh_ref[core], fl_ref[core], high, low)
        total = jnp.concatenate([sz_ref[...]] * wide, axis=1) + sq_ref[pl.ds(i, 1), :]
        keep = total > 0.0
        value = jnp.concatenate([az_ref[...]] * wide, axis=1) * col_ref[pl.ds(i, 1), :] / jnp.where(keep, total, 1.0)
        green = jnp.where(keep, value, 0.0)
        high, low = split(coef * jnp.concatenate([green, green], axis=0))
        back = dot3(bh_ref[...], bl_ref[...], high, low)
        for j in range(PACK):
            pot_ref[PACK * i + j, :, :LANES] = back[:, j * LANES : (j + 1) * LANES]
            tail = back[:, (PACK + j // 2) * LANES : (PACK + j // 2 + 1) * LANES]
            pot_ref[PACK * i + j, :, LANES:] = pltpu.roll(tail, LANES - part, 1) if j % 2 else tail
        return carry

    lax.fori_loop(0, modes // PACK, convolve, 0)
    span = 4 * 8
    wave_h[half:] = jnp.zeros((2 * LANES - half, 2 * atoms), BF16)
    wave_l[half:] = jnp.zeros((2 * LANES - half, 2 * atoms), BF16)
    ky = lax.broadcasted_iota(jnp.int32, (half, atoms), 0).astype(F32)
    mode = lax.broadcasted_iota(jnp.int32, (modes, atoms), 0)
    sine = mode >= kx_local
    kx = (kx_first + jnp.where(sine, mode - kx_local, mode)).astype(F32)
    x_shift = jnp.where(sine, points - points // 4, points).astype(F32)

    def slab(p, carry):
        qm = jnp.concatenate([qm_ref[2 * p], qm_ref[2 * p + 1]], axis=1)
        values, slopes = spline_rows(qm)
        table = [qm[0:1], qm[1:2], qm[2:3]]
        for d in range(3, 6):
            for part in (values, slopes):
                table += [v[d : d + 1] for v in part]
        row = lambda i: table[i]
        cosine, sinus = trig(ky * (2.0 * row(1) + 1.0) + y_shift.astype(F32), 2 * points)
        for k, at in ((0, 11), (1, 15)):
            real = imag = None
            for c in range(ORDER):
                sc = jnp.concatenate([step_ref[c]] * (atoms // LANES), axis=1)
                ss = jnp.concatenate([step_ref[ORDER + c]] * (atoms // LANES), axis=1)
                real = row(at + c) * sc if real is None else real + row(at + c) * sc
                imag = row(at + c) * ss if imag is None else imag + row(at + c) * ss
            high, low = split(cosine * real - sinus * imag)
            wave_h[0:half, k * atoms : (k + 1) * atoms] = high
            wave_l[0:half, k * atoms : (k + 1) * atoms] = low
        plain_x = slope_x = jnp.zeros((modes, atoms), F32)
        for c in range(ORDER):
            wave, _ = trig(kx * (row(2) + float(c)) + x_shift, points)
            plain_x += row(19 + c) * wave
            slope_x += row(23 + c) * wave
        wx_ref[0] = plain_x
        wx_ref[1] = slope_x
        z_first = pl.multiple_of(p * z_local, 8)
        acc_ref[...] = jnp.zeros_like(acc_ref)
        for g in range(modes // 8):
            tiles = [pot_ref[g * 8 + i, pl.ds(z_first, span), :] for i in range(8)]
            high, low = split(jnp.concatenate(tiles, axis=0))
            along = dot3(high, low, wave_h[...], wave_l[...])
            for i in range(8):
                r = g * 8 + i
                value, slope = along[i * span : (i + 1) * span, :atoms], along[i * span : (i + 1) * span, atoms:]
                wx, dx = wx_ref[0, r : r + 1], wx_ref[1, r : r + 1]
                acc_ref[0] += value * wx
                acc_ref[1] += slope * wx
                acc_ref[2] += value * dx
        off = lax.broadcasted_iota(jnp.int32, (span, atoms), 0) + z_first - row(0).astype(jnp.int32)
        wz = dz = jnp.zeros((span, atoms), F32)
        for a in range(ORDER):
            wz = jnp.where(off == a, row(3 + a), wz)
            dz = jnp.where(off == a, row(7 + a), dz)
        total = lambda v: jnp.sum(v, axis=0, keepdims=True)
        found = jnp.concatenate(
            [total(acc_ref[0] * dz), total(acc_ref[1] * wz), total(acc_ref[2] * wz), jnp.zeros((5, atoms), F32)], axis=0)
        out_ref[2 * p] = found[:, : atoms // 2]
        out_ref[2 * p + 1] = found[:, atoms // 2 :]
        return carry

    lax.fori_loop(0, slabs, slab, 0)


def spline_rows(frac):
    remain = 1.0 - frac
    square = frac * frac
    cubed = square * frac
    values = [
        remain * remain * remain / 6.0,
        (3.0 * cubed - 6.0 * square + 4.0) / 6.0,
        (-3.0 * cubed + 3.0 * square + 3.0 * frac + 1.0) / 6.0,
        cubed / 6.0,
    ]
    slopes = [
        -0.5 * remain * remain,
        (3.0 * square - 4.0 * frac) / 2.0,
        (-3.0 * square + 2.0 * frac + 1.0) / 2.0,
        0.5 * square,
    ]
    return values, slopes


def solve(lines, other, here, qm_all, kx_index, points):
    tiles, slab_half, deep, lanes = other.shape
    kx_local = kx_index.shape[0]
    modes = 2 * kx_local
    half = points // 2
    slabs, atoms = qm_all.shape[0] // 2, 2 * qm_all.shape[2]
    z_local = points // slabs
    z_used = z_local + ORDER - 1
    k = np.arange(half)

    def waves(z):
        angle = 2.0 * np.pi / points * ((k[:, None] * z[None, :]) % points)
        return np.concatenate([np.cos(angle), np.sin(angle)], axis=0)

    core, pair, plane = np.meshgrid(np.arange(2), np.arange(slabs // 2), np.arange(z_used), indexing="ij")
    cells = (((pair * 2 + core) * z_local + plane) % points).reshape(2, -1)
    fh, fl = split_table(np.stack([waves(cells.reshape(-1)), waves(cells[::-1].reshape(-1))]))
    reach = points + 8
    bh, bl = split_table(waves(np.arange(reach) % points).T)

    def parts_of(index):
        square, spline, _ = moduli(index, points)
        decay = jnp.exp(-(math.pi * math.pi / (SPLITTING * SPLITTING)) * square)
        return square, spline * decay * jnp.where(index == 0, 1.0, 2.0)

    z_sq, z_fac = parts_of(jnp.asarray(k, jnp.int32))
    x_sq, x_fac = parts_of(jnp.concatenate([kx_index, kx_index]))

    def packed(table):
        table = table.reshape(modes // PACK, PACK, half)
        head = table[:, :, :lanes].reshape(modes // PACK, PACK * lanes)
        return jnp.concatenate([head, table[:, :, lanes:].reshape(modes // PACK, -1)], axis=1)

    col = packed(x_fac[:, None] * z_fac[None, :] * (1.0 / (math.pi * float(points) ** 3)))
    sq = packed(x_sq[:, None] + z_sq[None, :])
    az = jnp.broadcast_to(z_fac[:, None], (half, lanes))
    sz = jnp.broadcast_to(z_sq[:, None], (half, lanes))
    vmem = pl.BlockSpec(memory_space=pltpu.VMEM)
    return pl.pallas_call(
        functools.partial(solve_kernel, points, kx_local),
        in_specs=[pl.BlockSpec(memory_space=pltpu.SMEM)] + [vmem] * 11,
        out_specs=vmem,
        out_shape=jax.ShapeDtypeStruct((2 * slabs, 8, atoms // 2), F32),
        scratch_shapes=[
            pltpu.VMEM((modes, reach, 2 * lanes), F32),
            pltpu.VMEM((2 * lanes, 2 * atoms), BF16),
            pltpu.VMEM((2 * lanes, 2 * atoms), BF16),
            pltpu.VMEM((2, modes, atoms), F32),
            pltpu.VMEM((3, 32, atoms), F32),
            pltpu.VMEM((2 * ORDER, half, lanes), F32),
        ],
        compiler_params=pltpu.CompilerParams(vmem_limit_bytes=VMEM_LIMIT),
        name="solve_interpolate",
    )(here, lines.reshape(2, tiles, slab_half * deep, lanes), other.reshape(tiles, slab_half * deep, lanes), fh, fl, bh, bl, az, sz, col, sq, qm_all)


def reduce_kernel(count_z, count_y, part_ref, out_ref, land_ref, send_sem, recv_sem):
    p = lax.axis_index("gz")
    y = lax.axis_index("gy")
    me = p * count_y + y
    total = count_z * count_y
    width = out_ref.shape[1]
    barrier = pltpu.get_barrier_semaphore()
    for d in range(1, total):
        other = lax.rem(me + d, total)
        pl.semaphore_signal(barrier, inc=1, device_id=(other // count_y, lax.rem(other, count_y)), device_id_type=MESH)
    pl.semaphore_wait(barrier, total - 1)
    for d in range(1, total):
        other = lax.rem(me + d, total)
        pltpu.make_async_remote_copy(
            src_ref=part_ref.at[other], dst_ref=land_ref.at[me], send_sem=send_sem, recv_sem=recv_sem,
            device_id=(other // count_y, lax.rem(other, count_y)), device_id_type=MESH).start()
    land_ref[me] = part_ref[me]
    pltpu.make_async_remote_copy(
        src_ref=land_ref.at[pl.ds(0, total - 1)], dst_ref=land_ref.at[pl.ds(0, total - 1)], send_sem=send_sem, recv_sem=recv_sem,
        device_id=(p, 1 - y), device_id_type=MESH).wait()
    out_ref[...] = jnp.sum(land_ref[...], axis=0)


def reduce_forces(partial, count_z, count_y):
    total, rows, width = partial.shape
    vmem = pl.BlockSpec(memory_space=pltpu.VMEM)
    return pl.pallas_call(
        functools.partial(reduce_kernel, count_z, count_y),
        in_specs=[vmem],
        out_specs=vmem,
        out_shape=jax.ShapeDtypeStruct((rows, width), F32),
        scratch_shapes=[pltpu.VMEM((total, rows, width), F32), pltpu.SemaphoreType.DMA, pltpu.SemaphoreType.DMA],
        compiler_params=pltpu.CompilerParams(collective_id=2, has_side_effects=True, vmem_limit_bytes=VMEM_LIMIT),
        name="reduce_forces",
    )(partial)


def fast_shards(spread_weights, spread_base, qm_base, qm_frac, qm_charge):
    points = GRID
    count_z = lax.axis_size("gz")
    count_y = lax.axis_size("gy")
    z_local, y_local = points // count_z, points // count_y
    kx_local = points // (RING * PLANE * 2)
    p = lax.axis_index("gz")
    q = lax.axis_index("gy")
    count = spread_weights.shape[1]
    qm_count = qm_base.shape[1]

    z_cell = spread_base[0] - p * z_local
    y_cell = spread_base[1] - q * y_local
    cells = jnp.stack([z_cell, y_cell, spread_base[2]]).astype(F32)
    table = jnp.concatenate(
        [spread_weights.reshape(ORDER, ORDER, ORDER, count).transpose(1, 0, 2, 3).reshape(ORDER**3, count),
         cells, jnp.zeros((5, count), F32)], axis=0)
    own = order_by(z_cell, table)
    qm = jnp.concatenate([qm_base.astype(F32), qm_frac, jnp.zeros((2, qm_count), F32)], axis=0)
    tab, qm_all = gather(own, qm)

    kx_first = ((p // 2) * count_y + q) * kx_local
    lines = spread(tab, kx_first, kx_local, z_local, y_local, points)
    other = swap(lines)
    kx_index = kx_first + jnp.arange(kx_local, dtype=jnp.int32)
    partial = solve(lines, other, jnp.stack([kx_first, p % 2]), qm_all, kx_index, points)
    forces = reduce_forces(partial, count_z, count_y)
    return -qm_charge * forces[:3]


def quick(mesh):
    return mesh.shape["gz"] == RING * PLANE and mesh.shape["gy"] == 2


def solution(mesh):
    in_specs = (
        P(None, ("gz", "gy")),
        P(None, ("gz", "gy")),
        P(None, ("gz", "gy")),
        P(None, ("gz", "gy")),
        P(("gz", "gy")),
    )
    out_specs = P(None, ("gz", "gy"))
    body = fast_shards if quick(mesh) else shards
    return jax.shard_map(body, mesh=mesh, in_specs=in_specs, out_specs=out_specs, check_vma=False)
```
